32 devices in a mesh: pz: 4 (over z), py: 2 (over y), px: 4 (over x, core).
Axes of the slice: x: 2, y: 2, z: 4, core: 2. Of those that a mesh axis runs over, the one named last changes fastest.
Arguments:
- shift_diag: float32 [2, 320, 160, 192], P(None, 'px', 'py', 'pz')
- rhs_field: float32 [2, 320, 160, 192], P(None, 'px', 'py', 'pz')
- x_start: float32 [2, 320, 160, 192], P(None, 'px', 'py', 'pz')
- cond_x: float32 [2, 320, 160, 192], P(None, 'px', 'py', 'pz')
- cond_y: float32 [2, 320, 160, 192], P(None, 'px', 'py', 'pz')
- cond_z: float32 [2, 320, 160, 192], P(None, 'px', 'py', 'pz')
Outputs:
- output 1: float32 [2, 320, 160, 192], P(None, 'px', 'py', 'pz')
- output 2: float32 [2, 21], replicated
All inputs are finite; a program needn't handle non-finite values.
Results may differ from the reference program's by a relative error of at most 0.001.
Values sent between devices are 32-bit elements.
A program may use at most 1 GiB of HBM per device.

```python
import jax
import jax.numpy as jnp
from jax import lax

GRID_X = 320
GRID_Y = 160
GRID_Z = 192
ITERS = 20


def setup_inputs(seed: int = 0) -> dict:
    base_key = jax.random.key(seed)
    sub_keys = jax.random.split(base_key, 6)
    field_shape = (2, GRID_X, GRID_Y, GRID_Z)
    shift_diag = 0.05 + 0.3 * jax.random.uniform(sub_keys[0], field_shape, jnp.float32)
    rhs_field = jax.random.normal(sub_keys[1], field_shape, jnp.float32)
    x_start = 0.5 * jax.random.normal(sub_keys[2], field_shape, jnp.float32)
    cond_x = 0.1 + 1.8 * jax.random.uniform(sub_keys[3], field_shape, jnp.float32)
    cond_y = 0.1 + 1.8 * jax.random.uniform(sub_keys[4], field_shape, jnp.float32)
    cond_z = 0.1 + 1.8 * jax.random.uniform(sub_keys[5], field_shape, jnp.float32)
    return {'shift_diag': shift_diag, 'rhs_field': rhs_field, 'x_start': x_start, 'cond_x': cond_x, 'cond_y': cond_y, 'cond_z': cond_z}


def face_term(field, conduct, axis_dim):
    planes = field.shape[axis_dim]
    face_flux = lax.slice_in_dim(conduct, 0, planes - 1, axis=axis_dim) * (lax.slice_in_dim(field, 0, planes - 1, axis=axis_dim) - lax.slice_in_dim(field, 1, planes, axis=axis_dim))
    widths = [(1, 1) if pos_dim == axis_dim else (0, 0) for pos_dim in range(field.ndim)]
    padded = jnp.pad(face_flux, widths)
    return lax.slice_in_dim(padded, 1, planes + 1, axis=axis_dim) - lax.slice_in_dim(padded, 0, planes, axis=axis_dim)


def apply_operator(field, shift_diag, cond_x, cond_y, cond_z):
    return shift_diag * field + face_term(field, cond_x, 0) + face_term(field, cond_y, 1) + face_term(field, cond_z, 2)


def solve_one(fields):
    shift_diag, rhs_field, x_start, cond_x, cond_y, cond_z = fields
    cell_count = GRID_X * GRID_Y * GRID_Z
    residual = rhs_field - apply_operator(x_start, shift_diag, cond_x, cond_y, cond_z)
    rho_start = jnp.sum(residual * residual)

    def cg_step(loop_state, unused):
        x_cur, res_cur, direction, rho_old, beta_coef = loop_state
        direction = res_cur + beta_coef * direction
        q_vec = apply_operator(direction, shift_diag, cond_x, cond_y, cond_z)
        alpha_step = rho_old / jnp.sum(direction * q_vec)
        x_cur = x_cur + alpha_step * direction
        res_cur = res_cur - alpha_step * q_vec
        rho_new = jnp.sum(res_cur * res_cur)
        return (x_cur, res_cur, direction, rho_new, rho_new / rho_old), jnp.sqrt(rho_new / cell_count)

    init_state = (x_start, residual, jnp.zeros_like(residual), rho_start, jnp.zeros_like(rho_start))
    final_state, res_tail = lax.scan(cg_step, init_state, None, length=ITERS)
    res_hist = jnp.concatenate([jnp.sqrt(rho_start / cell_count)[None], res_tail])
    return final_state[0], res_hist


def reference(shift_diag, rhs_field, x_start, cond_x, cond_y, cond_z):
    x_final, res_hist = lax.map(solve_one, (shift_diag, rhs_field, x_start, cond_x, cond_y, cond_z))
    return x_final, res_hist
```

```python
import functools

import jax
import jax.numpy as jnp
from jax import lax
from jax.experimental import pallas as pl
from jax.experimental.pallas import tpu as pltpu
from jax.sharding import PartitionSpec as P

ITERS = 20
AXES = ('pz', 'py', 'px')
MESH = pl.DeviceIdType.MESH
XB, YB, ZB = 16, 8, 8


def kernel(sizes, dims, s_hbm, b_hbm, x_hbm, kx_hbm, ky_hbm, kz_hbm, xo_hbm, hist_ref,
           stage, r, p, q, x, s, kx, ky, kz, fx, tmp,
           xs, xr, ys, yr, zs, zr, kxs, kxr, kys, kyr, kzs, kzr,
           dots, rho, hist,
           in_sem, out_sem, dot_send, dot_recv, halo_send, halo_recv, k_send, k_recv):
    nz_dev, ny_dev, nx_dev = sizes
    n_dev = nz_dev * ny_dev * nx_dev
    XI, YI, ZI, cells = dims
    pz, py, px = (lax.axis_index(a) for a in AXES)
    me = (pz * ny_dev + py) * nx_dev + px
    lane = lax.broadcasted_iota(jnp.int32, (8, 128), 1)
    sub = lax.broadcasted_iota(jnp.int32, (8, 128), 0)
    lane_z = lax.rem(lane, ZB)
    lane_x = lax.div(lane, ZB)
    row_lane = lax.broadcasted_iota(jnp.int32, (1, 128), 1)

    arrays = (x_hbm, kx_hbm, ky_hbm, kz_hbm, s_hbm, b_hbm)

    def in_copy(a, c):
        return pltpu.make_async_copy(arrays[a].at[c], stage.at[a, c], in_sem.at[a, c])

    for a in range(6):
        for c in range(2):
            in_copy(a, c).start()

    for ref in (xr, yr, zr, kxr, kyr, kzr):
        ref[...] = jnp.zeros(ref.shape, ref.dtype)

    def target(off):
        t = lax.rem(me + off, n_dev)
        rest = lax.rem(t, ny_dev * nx_dev)
        return (lax.div(t, ny_dev * nx_dev), lax.div(rest, nx_dev), lax.rem(rest, nx_dev))

    def each_other(fn):
        def step(i, _):
            fn(target(i))
            return 0
        lax.fori_loop(1, n_dev, step, 0, unroll=True)

    barrier = pltpu.get_barrier_semaphore()
    each_other(lambda dev: pl.semaphore_signal(barrier, inc=1, device_id=dev, device_id_type=MESH))
    pl.semaphore_wait(barrier, n_dev - 1)

    def unrolled(n, fn):
        def step(i, _):
            fn(i)
            return 0
        lax.fori_loop(0, n, step, 0, unroll=True)

    ysl, zsl = slice(1, YI + 1), slice(1, ZI + 1)
    xsl = slice(1, XI + 1)

    def relayout(a, stores):
        def system(c, _):
            in_copy(a, c).wait()

            def plane(xi, _):
                def load(zi):
                    rows = stage[a, c, :, xi, pl.ds(zi, ZB, stride=ZI), :]
                    tmp[zi] = rows.reshape(128, rows.shape[-1]).T
                unrolled(ZI, load)
                unrolled(ZI, lambda zi: unrolled(YI, lambda yi: stores(c, xi, yi, zi, tmp[zi, pl.ds(yi, YB, stride=YI), :])))
                return 0
            return lax.fori_loop(0, XI, plane, 0)
        lax.fori_loop(0, 2, system, 0)

    def pack_x(get, shift, put):
        acc = pltpu.roll(get(0), shift, 2) if shift else get(0)
        for j in range(1, YI):
            acc = jnp.where(lane_x == j, pltpu.roll(get(j), (shift + ZB * j) % 128, 2), acc)
        put(acc)

    def pack_z(get, src_zb, put):
        acc = pltpu.roll(get(0), (-src_zb) % 128, 2) if src_zb else get(0)
        for j in range(1, XI):
            v = get(j)
            acc = jnp.where(lane_z == j, pltpu.roll(v, (j - src_zb) % 128, 2) if j != src_zb else v, acc)
        put(acc)

    def ghost_x(v, packed, j, low):
        dst = 0 if low else XB - 1
        moved = pltpu.roll(v, ZB if low else 128 - ZB, 2)
        move = (ZB * (dst - j)) % 128
        return jnp.where(lane_x == dst, pltpu.roll(packed, move, 2) if move else packed, moved)

    def ghost_z(v, packed, j, low):
        dst = 0 if low else ZB - 1
        moved = pltpu.roll(v, 1 if low else 127, 2)
        move = (dst - j) % 128
        return jnp.where(lane_z == dst, pltpu.roll(packed, move, 2) if move else packed, moved)

    def ghost_y(v, rows, low):
        dst = 0 if low else YB - 1
        moved = pltpu.roll(v, 1 if low else YB - 1, v.ndim - 2)
        return jnp.where(sub == dst, jnp.broadcast_to(rows, v.shape), moved)

    def pack_field(f, c):
        def put(ref, d):
            def put_(v):
                ref[d, c] = v
            return put_
        pack_x(lambda yi: f[c, 1, yi + 1, zsl], 0, put(xs, 0))
        pack_x(lambda yi: f[c, XI, yi + 1, zsl], ZB, put(xs, 1))
        pack_z(lambda xi: f[c, xi + 1, ysl, 1], 0, put(zs, 0))
        pack_z(lambda xi: f[c, xi + 1, ysl, ZI], ZB - 1, put(zs, 1))
        ys[0, c] = f[c, xsl, 1, zsl, 0:1, :]
        ys[1, c] = f[c, xsl, YI, zsl, YB - 1:YB, :]

    def ghost_field(f, c, w):
        for yi in range(YI):
            f[c, 0, yi + 1, zsl] = ghost_x(f[c, XI, yi + 1, zsl], xr[w, 0, c], yi, True)
            f[c, XI + 1, yi + 1, zsl] = ghost_x(f[c, 1, yi + 1, zsl], xr[w, 1, c], yi, False)
        for xi in range(XI):
            f[c, xi + 1, ysl, 0] = ghost_z(f[c, xi + 1, ysl, ZI], zr[w, 0, c], xi, True)
            f[c, xi + 1, ysl, ZI + 1] = ghost_z(f[c, xi + 1, ysl, 1], zr[w, 1, c], xi, False)
        f[c, xsl, 0, zsl] = ghost_y(f[c, xsl, YI, zsl], yr[w, 0, c], True)
        f[c, xsl, YI + 1, zsl] = ghost_y(f[c, xsl, 1, zsl], yr[w, 1, c], False)

    lower = ((px > 0, (pz, py, px - 1)), (py > 0, (pz, py - 1, px)), (pz > 0, (pz - 1, py, px)))
    upper = ((px < nx_dev - 1, (pz, py, px + 1)), (py < ny_dev - 1, (pz, py + 1, px)), (pz < nz_dev - 1, (pz + 1, py, px)))

    def halo_copies(w):
        out = []
        for axis, (src, dst) in enumerate(((xs, xr), (ys, yr), (zs, zr))):
            for d in range(2):
                ok_send, dev = (lower, upper)[d][axis]
                ok_recv, _ = (upper, lower)[d][axis]
                cp = pltpu.make_async_remote_copy(
                    src_ref=src.at[d], dst_ref=dst.at[w, 1 - d], send_sem=halo_send.at[w, 2 * axis + d],
                    recv_sem=halo_recv.at[w, 2 * axis + d], device_id=dev, device_id_type=MESH)
                out.append((ok_send, ok_recv, cp))
        return out

    def k_copies():
        out = []
        for axis, (src, dst) in enumerate(((kxs, kxr), (kys, kyr), (kzs, kzr))):
            cp = pltpu.make_async_remote_copy(
                src_ref=src, dst_ref=dst, send_sem=k_send.at[axis], recv_sem=k_recv.at[axis],
                device_id=upper[axis][1], device_id_type=MESH)
            out.append((upper[axis][0], lower[axis][0], cp))
        return out

    def start_all(copies):
        for ok_send, _, cp in copies:
            pl.when(ok_send)(cp.start)

    def wait_all(copies):
        for ok_send, ok_recv, cp in copies:
            pl.when(ok_send)(cp.wait_send)
            pl.when(ok_recv)(cp.wait_recv)

    def send_dot(kind, c, acc):
        acc = jnp.sum(acc, axis=0)
        dots[kind, c, me] = jnp.sum(acc, axis=0, keepdims=True)
        each_other(lambda dev: pltpu.make_async_remote_copy(
            src_ref=dots.at[kind, c, me], dst_ref=dots.at[kind, c, me], send_sem=dot_send.at[kind, c],
            recv_sem=dot_recv.at[kind, c], device_id=dev, device_id_type=MESH).start())

    def wait_dot(kind, c):
        rows = dots.at[kind, c, pl.ds(0, n_dev - 1)]
        cp = pltpu.make_async_remote_copy(
            src_ref=rows, dst_ref=rows, send_sem=dot_send.at[kind, c], recv_sem=dot_recv.at[kind, c],
            device_id=(pz, py, px), device_id_type=MESH)
        cp.wait_recv()
        cp.wait_send()
        terms = [dots[kind, c, d] for d in range(n_dev)]
        while len(terms) > 1:
            terms = [terms[i] + terms[i + 1] for i in range(0, len(terms), 2)]
        total = jnp.sum(terms[0], axis=1, keepdims=True)
        return jnp.broadcast_to(total, (1, 128))

    def phase_a(c, beta):
        if beta is not None:
            beta = jnp.broadcast_to(beta, (8, 128))

        def new_p(*idx):
            if beta is not None:
                p[idx] = r[idx] + beta * p[idx]

        def head(yi):
            new_p(c, 0, yi + 1, zsl)
            new_p(c, 1, yi + 1, zsl)
            fx[yi] = kx[c, 0, yi] * (p[c, 0, yi + 1, zsl] - p[c, 1, yi + 1, zsl])
        unrolled(YI, head)

        def plane(xi, acc):
            new_p(c, xi + 1, ysl, 0)
            new_p(c, xi + 1, ysl, ZI + 1)
            new_p(c, xi + 1, 0, zsl)
            new_p(c, xi + 1, YI + 1, zsl)
            pc = p[c, xi + 1, 1, zsl]
            fy_lo = ky[c, xi, 0] * (p[c, xi + 1, 0, zsl] - pc)

            def line(yi, carry):
                acc, pc, fy_lo = carry
                new_p(c, xi + 2, yi + 1, zsl)
                py_hi = p[c, xi + 1, yi + 2, zsl]
                fx_lo = fx[yi]
                fx_hi = kx[c, xi + 1, yi] * (pc - p[c, xi + 2, yi + 1, zsl])
                fx[yi] = fx_hi
                fy_hi = ky[c, xi, yi + 1] * (pc - py_hi)
                fz = kz[c, xi, yi] * (p[c, xi + 1, yi + 1, :ZI + 1] - p[c, xi + 1, yi + 1, 1:])
                out = s[c, xi, yi] * pc + (fx_hi - fx_lo) + (fy_hi - fy_lo) + (fz[1:] - fz[:-1])
                q[c, xi, yi] = out
                return acc + pc * out, py_hi, fy_hi
            return lax.fori_loop(0, YI, line, (acc, pc, fy_lo), unroll=True)[0]
        return lax.fori_loop(0, XI, plane, jnp.zeros((ZI, 8, 128), jnp.float32))

    def phase_b(c, alpha):
        if alpha is not None:
            alpha = jnp.broadcast_to(alpha, (8, 128))

        def plane(xi, acc):
            def line(yi, acc):
                step = q[c, xi, yi] if alpha is None else alpha * q[c, xi, yi]
                v = r[c, xi + 1, yi + 1, zsl] - step
                r[c, xi + 1, yi + 1, zsl] = v
                return acc + v * v
            return lax.fori_loop(0, YI, line, acc, unroll=True)
        return lax.fori_loop(0, XI, plane, jnp.zeros((ZI, 8, 128), jnp.float32))

    def phase_x(c, alpha):
        alpha = jnp.broadcast_to(alpha, (8, 128))

        def plane(xi, _):
            x[c, xi] = x[c, xi] + alpha * p[c, xi + 1, ysl, zsl]
            return 0
        lax.fori_loop(0, XI, plane, 0)

    def both(fn):
        def system(c, _):
            fn(c)
            return 0
        lax.fori_loop(0, 2, system, 0)

    def put_x(c, xi, yi, zi, v):
        p[c, xi + 1, yi + 1, zi + 1] = v
        x[c, xi, yi, zi] = v
    relayout(0, put_x)
    both(lambda c: pack_field(p, c))
    start_all(halo_copies(1))

    def put_to(ref, ox, oy, oz):
        def put(c, xi, yi, zi, v):
            ref[c, xi + ox, yi + oy, zi + oz] = v
        return put
    relayout(1, put_to(kx, 1, 0, 0))
    relayout(2, put_to(ky, 0, 1, 0))
    relayout(3, put_to(kz, 0, 0, 1))

    def pack_k(c):
        def put(ref):
            def put_(v):
                ref[c] = v
            return put_
        pack_x(lambda yi: kx[c, XI, yi], ZB, put(kxs))
        pack_z(lambda xi: kz[c, xi, :, ZI], ZB - 1, put(kzs))
        kys[c] = ky[c, :, YI, :, YB - 1:YB, :]
    both(pack_k)
    start_all(k_copies())
    relayout(4, put_to(s, 0, 0, 0))
    relayout(5, put_to(r, 1, 1, 1))
    wait_all(halo_copies(1))
    both(lambda c: ghost_field(p, c, 1))
    wait_all(k_copies())

    def ghost_k(c):
        def edge(cond, v):
            return jnp.where(cond, 0.0, v)
        for yi in range(YI):
            v = kx[c, XI, yi]
            kx[c, 0, yi] = ghost_x(v, kxr[c], yi, True)
            kx[c, XI, yi] = edge(jnp.logical_and(lane_x == XB - 1, px == nx_dev - 1), v)
        for xi in range(XI):
            v = kz[c, xi, :, ZI]
            kz[c, xi, :, 0] = ghost_z(v, kzr[c], xi, True)
            kz[c, xi, :, ZI] = edge(jnp.logical_and(lane_z == ZB - 1, pz == nz_dev - 1), v)
        v = ky[c, :, YI]
        ky[c, :, 0] = ghost_y(v, kyr[c], True)
        ky[c, :, YI] = edge(jnp.logical_and(sub == YB - 1, py == ny_dev - 1), v)
    both(ghost_k)

    for c in range(2):
        phase_a(c, None)
        send_dot(1, c, phase_b(c, None))
    both(lambda c: pack_field(r, c))
    start_all(halo_copies(0))
    rho[...] = jnp.ones(rho.shape, jnp.float32)
    hist[...] = jnp.zeros(hist.shape, jnp.float32)

    def new_rho(c, k):
        total = wait_dot(1, c)
        ratio = total / rho[c]
        rho[c] = total
        hist[c] = jnp.where(row_lane == k, total, hist[c])
        return ratio

    def iteration(k, _):
        wait_all(halo_copies(0))
        both(lambda c: ghost_field(r, c, 0))
        for c in range(2):
            beta = new_rho(c, k)
            beta = jnp.where(k == 0, 0.0, beta)
            send_dot(0, c, phase_a(c, beta))
        alphas = []
        for c in range(2):
            alpha = rho[c] / wait_dot(0, c)
            alphas.append(alpha)
            send_dot(1, c, phase_b(c, alpha))

        @pl.when(k < ITERS - 1)
        def _():
            both(lambda c: pack_field(r, c))
            start_all(halo_copies(0))
        for c in range(2):
            phase_x(c, alphas[c])
        return 0
    lax.fori_loop(0, ITERS, iteration, 0)

    def system_out(c, _):
        def plane(xi, _):
            def gather(zi):
                def line(yi):
                    tmp[zi, pl.ds(yi, YB, stride=YI), :] = x[c, xi, yi, zi]
                unrolled(YI, line)
            unrolled(ZI, gather)

            def put(zi):
                stage[0, c, :, xi, pl.ds(zi, ZB, stride=ZI), :] = tmp[zi].T.reshape(XB, ZB, tmp.shape[1])
            unrolled(ZI, put)
            return 0
        lax.fori_loop(0, XI, plane, 0)
        pltpu.make_async_copy(stage.at[0, c], xo_hbm.at[c], out_sem.at[c]).start()
        return 0
    lax.fori_loop(0, 2, system_out, 0)
    for c in range(2):
        new_rho(c, ITERS)
        hist_ref[c:c + 1, :] = jnp.sqrt(hist[c] / cells)[:, :ITERS + 1]
    for c in range(2):
        pltpu.make_async_copy(stage.at[0, c], xo_hbm.at[c], out_sem.at[c]).wait()


def solution(mesh):
    sizes = tuple(mesh.shape[a] for a in AXES)
    n_dev = sizes[0] * sizes[1] * sizes[2]
    field_spec = P(None, 'px', 'py', 'pz')

    def local_solve(*args):
        _, nx, ny, nz = args[0].shape
        XI, YI, ZI = nx // XB, ny // YB, nz // ZB
        cells = float(nx * ny * nz * n_dev)
        f32 = jnp.float32
        rows = (XI, ZI, 1, 128)

        def vregs(*lead):
            return pltpu.VMEM(lead + (8, 128), f32)
        hbm = pl.BlockSpec(memory_space=pl.ANY)
        args = [jnp.swapaxes(a, 2, 3).reshape(2, XB, XI, nz, ny) for a in args]
        x_out, hist = pl.pallas_call(
            functools.partial(kernel, sizes, (XI, YI, ZI, cells)),
            out_shape=(jax.ShapeDtypeStruct((2, XB, XI, nz, ny), f32), jax.ShapeDtypeStruct((2, ITERS + 1), f32)),
            in_specs=[hbm] * 6,
            out_specs=(hbm, pl.BlockSpec(memory_space=pltpu.VMEM)),
            scratch_shapes=[
                pltpu.VMEM((6, 2, XB, XI, nz, ny), f32),
                vregs(2, XI + 2, YI + 2, ZI + 2), vregs(2, XI + 2, YI + 2, ZI + 2),
                vregs(2, XI, YI, ZI), vregs(2, XI, YI, ZI), vregs(2, XI, YI, ZI),
                vregs(2, XI + 1, YI, ZI), vregs(2, XI, YI + 1, ZI), vregs(2, XI, YI, ZI + 1),
                vregs(YI, ZI), pltpu.VMEM((ZI, ny, 128), f32),
                vregs(2, 2, ZI), vregs(2, 2, 2, ZI), pltpu.VMEM((2, 2) + rows, f32), pltpu.VMEM((2, 2, 2) + rows, f32),
                vregs(2, 2, YI), vregs(2, 2, 2, YI),
                vregs(2, ZI), vregs(2, ZI), pltpu.VMEM((2,) + rows, f32), pltpu.VMEM((2,) + rows, f32),
                vregs(2, YI), vregs(2, YI),
                pltpu.VMEM((2, 2, n_dev, 1, 128), f32), pltpu.VMEM((2, 1, 128), f32), pltpu.VMEM((2, 1, 128), f32),
                pltpu.SemaphoreType.DMA((6, 2)), pltpu.SemaphoreType.DMA((2,)),
                pltpu.SemaphoreType.DMA((2, 2)), pltpu.SemaphoreType.DMA((2, 2)),
                pltpu.SemaphoreType.DMA((2, 6)), pltpu.SemaphoreType.DMA((2, 6)),
                pltpu.SemaphoreType.DMA((3,)), pltpu.SemaphoreType.DMA((3,)),
            ],
            compiler_params=pltpu.CompilerParams(collective_id=0, has_side_effects=True, vmem_limit_bytes=67043328),
            name='cg',
        )(*args)
        return jnp.swapaxes(x_out.reshape(2, nx, nz, ny), 2, 3), hist

    return jax.shard_map(local_solve, mesh=mesh, in_specs=(field_spec,) * 6, out_specs=(field_spec, P(None, None)), check_vma=False)
```

```python
import functools

import jax
import jax.numpy as jnp
from jax import lax
from jax.experimental import pallas as pl
from jax.experimental.pallas import tpu as pltpu
from jax.sharding import PartitionSpec as P

ITERS = 20
AXES = ('pz', 'py', 'px')
MESH = pl.DeviceIdType.MESH
XB, YB, ZB = 16, 8, 8


def kernel(sizes, dims, s_hbm, b_hbm, x_hbm, kx_hbm, ky_hbm, kz_hbm, xo_hbm, hist_ref,
           stage, r, p, q, x, s, kx, ky, kz, fx, tmp,
           xs, xr, ys, yr, zs, zr, kxs, kxr, kys, kyr, kzs, kzr,
           dots, rho, hist,
           in_sem, out_sem, dot_send, dot_recv, halo_send, halo_recv, k_send, k_recv):
    nz_dev, ny_dev, nx_dev = sizes
    n_dev = nz_dev * ny_dev * nx_dev
    XI, YI, ZI, cells = dims
    pz, py, px = (lax.axis_index(a) for a in AXES)
    me = (pz * ny_dev + py) * nx_dev + px
    lane = lax.broadcasted_iota(jnp.int32, (8, 128), 1)
    sub = lax.broadcasted_iota(jnp.int32, (8, 128), 0)
    lane_z = lax.rem(lane, ZB)
    lane_x = lax.div(lane, ZB)
    row_lane = lax.broadcasted_iota(jnp.int32, (1, 128), 1)

    arrays = (x_hbm, kx_hbm, ky_hbm, kz_hbm, s_hbm, b_hbm)

    def in_copy(a, c):
        return pltpu.make_async_copy(arrays[a].at[c], stage.at[a, c], in_sem.at[a, c])

    for a in range(6):
        for c in range(2):
            in_copy(a, c).start()

    for ref in (xr, yr, zr, kxr, kyr, kzr):
        ref[...] = jnp.zeros(ref.shape, ref.dtype)

    def target(off):
        t = lax.rem(me + off, n_dev)
        rest = lax.rem(t, ny_dev * nx_dev)
        return (lax.div(t, ny_dev * nx_dev), lax.div(rest, nx_dev), lax.rem(rest, nx_dev))

    def each_other(fn):
        def step(i, _):
            fn(target(i))
            return 0
        lax.fori_loop(1, n_dev, step, 0, unroll=True)

    barrier = pltpu.get_barrier_semaphore()
    each_other(lambda dev: pl.semaphore_signal(barrier, inc=1, device_id=dev, device_id_type=MESH))
    pl.semaphore_wait(barrier, n_dev - 1)

    def unrolled(n, fn):
        def step(i, _):
            fn(i)
            return 0
        lax.fori_loop(0, n, step, 0, unroll=True)

    ysl, zsl = slice(1, YI + 1), slice(1, ZI + 1)
    xsl = slice(1, XI + 1)

    def relayout(a, stores):
        def system(c, _):
            in_copy(a, c).wait()

            def plane(xi, _):
                def load(zi):
                    rows = stage[a, c, :, xi, pl.ds(zi, ZB, stride=ZI), :]
                    tmp[zi] = rows.reshape(128, rows.shape[-1]).T
                unrolled(ZI, load)
                unrolled(ZI, lambda zi: unrolled(YI, lambda yi: stores(c, xi, yi, zi, tmp[zi, pl.ds(yi, YB, stride=YI), :])))
                return 0
            return lax.fori_loop(0, XI, plane, 0)
        lax.fori_loop(0, 2, system, 0)

    def pack_x(get, shift, put):
        acc = pltpu.roll(get(0), shift, 2) if shift else get(0)
        for j in range(1, YI):
            acc = jnp.where(lane_x == j, pltpu.roll(get(j), (shift + ZB * j) % 128, 2), acc)
        put(acc)

    def pack_z(get, src_zb, put):
        acc = pltpu.roll(get(0), (-src_zb) % 128, 2) if src_zb else get(0)
        for j in range(1, XI):
            v = get(j)
            acc = jnp.where(lane_z == j, pltpu.roll(v, (j - src_zb) % 128, 2) if j != src_zb else v, acc)
        put(acc)

    def ghost_x(v, packed, j, low):
        dst = 0 if low else XB - 1
        moved = pltpu.roll(v, ZB if low else 128 - ZB, 2)
        move = (ZB * (dst - j)) % 128
        return jnp.where(lane_x == dst, pltpu.roll(packed, move, 2) if move else packed, moved)

    def ghost_z(v, packed, j, low):
        dst = 0 if low else ZB - 1
        moved = pltpu.roll(v, 1 if low else 127, 2)
        move = (dst - j) % 128
        return jnp.where(lane_z == dst, pltpu.roll(packed, move, 2) if move else packed, moved)

    def ghost_y(v, rows, low):
        dst = 0 if low else YB - 1
        moved = pltpu.roll(v, 1 if low else YB - 1, v.ndim - 2)
        return jnp.where(sub == dst, jnp.broadcast_to(rows, v.shape), moved)

    def pack_field(f, c, o):
        def put(ref, d):
            def put_(v):
                ref[d, c] = v
            return put_
        xa, ya, za = slice(o, o + XI), slice(o, o + YI), slice(o, o + ZI)
        pack_x(lambda yi: f[c, o, yi + o, za], 0, put(xs, 0))
        pack_x(lambda yi: f[c, XI - 1 + o, yi + o, za], ZB, put(xs, 1))
        pack_z(lambda xi: f[c, xi + o, ya, o], 0, put(zs, 0))
        pack_z(lambda xi: f[c, xi + o, ya, ZI - 1 + o], ZB - 1, put(zs, 1))
        ys[0, c] = f[c, xa, o, za, 0:1, :]
        ys[1, c] = f[c, xa, YI - 1 + o, za, YB - 1:YB, :]

    def ghost_field(f, c, w):
        for yi in range(YI):
            f[c, 0, yi + 1, zsl] = ghost_x(f[c, XI, yi + 1, zsl], xr[w, 0, c], yi, True)
            f[c, XI + 1, yi + 1, zsl] = ghost_x(f[c, 1, yi + 1, zsl], xr[w, 1, c], yi, False)
        for xi in range(XI):
            f[c, xi + 1, ysl, 0] = ghost_z(f[c, xi + 1, ysl, ZI], zr[w, 0, c], xi, True)
            f[c, xi + 1, ysl, ZI + 1] = ghost_z(f[c, xi + 1, ysl, 1], zr[w, 1, c], xi, False)
        f[c, xsl, 0, zsl] = ghost_y(f[c, xsl, YI, zsl], yr[w, 0, c], True)
        f[c, xsl, YI + 1, zsl] = ghost_y(f[c, xsl, 1, zsl], yr[w, 1, c], False)

    lower = ((px > 0, (pz, py, px - 1)), (py > 0, (pz, py - 1, px)), (pz > 0, (pz - 1, py, px)))
    upper = ((px < nx_dev - 1, (pz, py, px + 1)), (py < ny_dev - 1, (pz, py + 1, px)), (pz < nz_dev - 1, (pz + 1, py, px)))

    def halo_copies(w):
        out = []
        for axis, (src, dst) in enumerate(((xs, xr), (ys, yr), (zs, zr))):
            for d in range(2):
                ok_send, dev = (lower, upper)[d][axis]
                ok_recv, _ = (upper, lower)[d][axis]
                cp = pltpu.make_async_remote_copy(
                    src_ref=src.at[d], dst_ref=dst.at[w, 1 - d], send_sem=halo_send.at[w, 2 * axis + d],
                    recv_sem=halo_recv.at[w, 2 * axis + d], device_id=dev, device_id_type=MESH)
                out.append((ok_send, ok_recv, cp))
        return out

    def k_copies():
        out = []
        for axis, (src, dst) in enumerate(((kxs, kxr), (kys, kyr), (kzs, kzr))):
            cp = pltpu.make_async_remote_copy(
                src_ref=src, dst_ref=dst, send_sem=k_send.at[axis], recv_sem=k_recv.at[axis],
                device_id=upper[axis][1], device_id_type=MESH)
            out.append((upper[axis][0], lower[axis][0], cp))
        return out

    def start_all(copies):
        for ok_send, _, cp in copies:
            pl.when(ok_send)(cp.start)

    def wait_all(copies):
        for ok_send, ok_recv, cp in copies:
            pl.when(ok_send)(cp.wait_send)
            pl.when(ok_recv)(cp.wait_recv)

    def send_dot(kind, c, acc):
        acc = jnp.sum(acc, axis=0)
        dots[kind, c, me] = jnp.sum(acc, axis=0, keepdims=True)
        each_other(lambda dev: pltpu.make_async_remote_copy(
            src_ref=dots.at[kind, c, me], dst_ref=dots.at[kind, c, me], send_sem=dot_send.at[kind, c],
            recv_sem=dot_recv.at[kind, c], device_id=dev, device_id_type=MESH).start())

    def wait_dot(kind, c):
        rows = dots.at[kind, c, pl.ds(0, n_dev - 1)]
        cp = pltpu.make_async_remote_copy(
            src_ref=rows, dst_ref=rows, send_sem=dot_send.at[kind, c], recv_sem=dot_recv.at[kind, c],
            device_id=(pz, py, px), device_id_type=MESH)
        cp.wait_recv()
        cp.wait_send()
        terms = [dots[kind, c, d] for d in range(n_dev)]
        while len(terms) > 1:
            terms = [terms[i] + terms[i + 1] for i in range(0, len(terms), 2)]
        total = jnp.sum(terms[0], axis=1, keepdims=True)
        return jnp.broadcast_to(total, (1, 128))

    def phase_a(c, beta):
        if beta is not None:
            beta = jnp.broadcast_to(beta, (8, 128))

        def new_p(*idx):
            if beta is not None:
                p[idx] = r[idx] + beta * p[idx]

        def head(yi):
            new_p(c, 0, yi + 1, zsl)
            new_p(c, 1, yi + 1, zsl)
            fx[yi] = kx[c, 0, yi] * (p[c, 0, yi + 1, zsl] - p[c, 1, yi + 1, zsl])
        unrolled(YI, head)

        def plane(xi, acc):
            new_p(c, xi + 1, ysl, 0)
            new_p(c, xi + 1, ysl, ZI + 1)
            new_p(c, xi + 1, 0, zsl)
            new_p(c, xi + 1, YI + 1, zsl)
            pc = p[c, xi + 1, 1, zsl]
            fy_lo = ky[c, xi, 0] * (p[c, xi + 1, 0, zsl] - pc)

            def line(yi, carry):
                acc, pc, fy_lo = carry
                new_p(c, xi + 2, yi + 1, zsl)
                py_hi = p[c, xi + 1, yi + 2, zsl]
                fx_lo = fx[yi]
                fx_hi = kx[c, xi + 1, yi] * (pc - p[c, xi + 2, yi + 1, zsl])
                fx[yi] = fx_hi
                fy_hi = ky[c, xi, yi + 1] * (pc - py_hi)
                fz = kz[c, xi, yi] * (p[c, xi + 1, yi + 1, :ZI + 1] - p[c, xi + 1, yi + 1, 1:])
                out = s[c, xi, yi] * pc + (fx_hi - fx_lo) + (fy_hi - fy_lo) + (fz[1:] - fz[:-1])
                q[c, xi, yi] = out
                return acc + pc * out, py_hi, fy_hi
            return lax.fori_loop(0, YI, line, (acc, pc, fy_lo), unroll=True)[0]
        return lax.fori_loop(0, XI, plane, jnp.zeros((ZI, 8, 128), jnp.float32))

    def phase_b(c, alpha):
        if alpha is not None:
            alpha = jnp.broadcast_to(alpha, (8, 128))

        def plane(xi, acc):
            def line(yi, acc):
                step = q[c, xi, yi] if alpha is None else alpha * q[c, xi, yi]
                v = r[c, xi + 1, yi + 1, zsl] - step
                r[c, xi + 1, yi + 1, zsl] = v
                return acc + v * v
            return lax.fori_loop(0, YI, line, acc, unroll=True)
        return lax.fori_loop(0, XI, plane, jnp.zeros((ZI, 8, 128), jnp.float32))

    def phase_x(c, alpha):
        alpha = jnp.broadcast_to(alpha, (8, 128))

        def plane(xi, _):
            x[c, xi] = x[c, xi] + alpha * p[c, xi + 1, ysl, zsl]
            return 0
        lax.fori_loop(0, XI, plane, 0)

    def both(fn):
        def system(c, _):
            fn(c)
            return 0
        lax.fori_loop(0, 2, system, 0)

    def put_x(c, xi, yi, zi, v):
        p[c, xi + 1, yi + 1, zi + 1] = v
        x[c, xi, yi, zi] = v
    relayout(0, put_x)
    both(lambda c: pack_field(p, c, 1))
    start_all(halo_copies(1))

    def put_to(ref, ox, oy, oz):
        def put(c, xi, yi, zi, v):
            ref[c, xi + ox, yi + oy, zi + oz] = v
        return put
    relayout(1, put_to(kx, 1, 0, 0))
    relayout(2, put_to(ky, 0, 1, 0))
    relayout(3, put_to(kz, 0, 0, 1))

    def pack_k(c):
        def put(ref):
            def put_(v):
                ref[c] = v
            return put_
        pack_x(lambda yi: kx[c, XI, yi], ZB, put(kxs))
        pack_z(lambda xi: kz[c, xi, :, ZI], ZB - 1, put(kzs))
        kys[c] = ky[c, :, YI, :, YB - 1:YB, :]
    both(pack_k)
    start_all(k_copies())
    relayout(4, put_to(s, 0, 0, 0))
    relayout(5, put_to(r, 1, 1, 1))
    wait_all(halo_copies(1))
    both(lambda c: ghost_field(p, c, 1))
    wait_all(k_copies())

    def ghost_k(c):
        def edge(cond, v):
            return jnp.where(cond, 0.0, v)
        for yi in range(YI):
            v = kx[c, XI, yi]
            kx[c, 0, yi] = ghost_x(v, kxr[c], yi, True)
            kx[c, XI, yi] = edge(jnp.logical_and(lane_x == XB - 1, px == nx_dev - 1), v)
        for xi in range(XI):
            v = kz[c, xi, :, ZI]
            kz[c, xi, :, 0] = ghost_z(v, kzr[c], xi, True)
            kz[c, xi, :, ZI] = edge(jnp.logical_and(lane_z == ZB - 1, pz == nz_dev - 1), v)
        v = ky[c, :, YI]
        ky[c, :, 0] = ghost_y(v, kyr[c], True)
        ky[c, :, YI] = edge(jnp.logical_and(sub == YB - 1, py == ny_dev - 1), v)
    both(ghost_k)

    for c in range(2):
        phase_a(c, None)
        send_dot(1, c, phase_b(c, None))
    both(lambda c: pack_field(r, c, 1))
    start_all(halo_copies(0))
    rho[...] = jnp.ones(rho.shape, jnp.float32)
    hist[...] = jnp.zeros(hist.shape, jnp.float32)
    wait_all(halo_copies(0))
    both(lambda c: ghost_field(r, c, 0))

    def new_rho(c, k):
        total = wait_dot(1, c)
        ratio = total / rho[c]
        rho[c] = total
        hist[c] = jnp.where(row_lane == k, total, hist[c])
        return ratio

    def iteration(k, _):
        slot = 2 + lax.rem(k, 2)
        for c in range(2):
            beta = new_rho(c, k)
            beta = jnp.where(k == 0, 0.0, beta)
            send_dot(0, c, phase_a(c, beta))

        @pl.when(k < ITERS - 1)
        def _():
            both(lambda c: pack_field(q, c, 0))
            start_all(halo_copies(slot))
        alphas = []
        for c in range(2):
            alpha = rho[c] / wait_dot(0, c)
            alphas.append(alpha)
            send_dot(1, c, phase_b(c, alpha))
        for c in range(2):
            phase_x(c, alphas[c])

        @pl.when(k < ITERS - 1)
        def _():
            wait_all(halo_copies(slot))
            for ref in (xr, yr, zr):
                for d in range(2):
                    for c in range(2):
                        ref[0, d, c] = ref[0, d, c] - alphas[c] * ref[slot, d, c]
            both(lambda c: ghost_field(r, c, 0))
        return 0
    lax.fori_loop(0, ITERS, iteration, 0)

    for c in range(2):
        pltpu.make_async_copy(x.at[c], xo_hbm.at[c], out_sem.at[c]).start()
    for c in range(2):
        new_rho(c, ITERS)
        hist_ref[c:c + 1, :] = jnp.sqrt(hist[c] / cells)[:, :ITERS + 1]
    for c in range(2):
        pltpu.make_async_copy(x.at[c], xo_hbm.at[c], out_sem.at[c]).wait()


def cell_order(dims, x_hbm, o_hbm, x, stage, tmp, in_sem, out_sem):
    XI, YI, ZI = dims
    for c in range(2):
        pltpu.make_async_copy(x_hbm.at[c], x.at[c], in_sem.at[c]).start()

    def out_copy(c, xi):
        return pltpu.make_async_copy(stage.at[c, :, xi], o_hbm.at[c, :, xi], out_sem.at[c, xi])

    for c in range(2):
        pltpu.make_async_copy(x_hbm.at[c], x.at[c], in_sem.at[c]).wait()

        def plane(xi, _):
            for zi in range(ZI):
                for yi in range(YI):
                    tmp[zi, pl.ds(yi, YB, stride=YI), :] = x[c, xi, yi, zi]
            for zi in range(ZI):
                stage[c, :, xi, pl.ds(zi, ZB, stride=ZI), :] = tmp[zi].T.reshape(XB, ZB, tmp.shape[1])
            out_copy(c, xi).start()
            return 0
        lax.fori_loop(0, XI, plane, 0)
    for c in range(2):
        for xi in range(XI):
            out_copy(c, xi).wait()


def solution(mesh):
    sizes = tuple(mesh.shape[a] for a in AXES)
    n_dev = sizes[0] * sizes[1] * sizes[2]
    field_spec = P(None, 'px', 'py', 'pz')

    def local_solve(*args):
        _, nx, ny, nz = args[0].shape
        XI, YI, ZI = nx // XB, ny // YB, nz // ZB
        cells = float(nx * ny * nz * n_dev)
        f32 = jnp.float32
        rows = (XI, ZI, 1, 128)

        def vregs(*lead):
            return pltpu.VMEM(lead + (8, 128), f32)
        hbm = pl.BlockSpec(memory_space=pl.ANY)
        args = [jnp.swapaxes(a, 2, 3).reshape(2, XB, XI, nz, ny) for a in args]
        x_out, hist = pl.pallas_call(
            functools.partial(kernel, sizes, (XI, YI, ZI, cells)),
            out_shape=(jax.ShapeDtypeStruct((2, XI, YI, ZI, 8, 128), f32), jax.ShapeDtypeStruct((2, ITERS + 1), f32)),
            in_specs=[hbm] * 6,
            out_specs=(hbm, pl.BlockSpec(memory_space=pltpu.VMEM)),
            scratch_shapes=[
                pltpu.VMEM((6, 2, XB, XI, nz, ny), f32),
                vregs(2, XI + 2, YI + 2, ZI + 2), vregs(2, XI + 2, YI + 2, ZI + 2),
                vregs(2, XI, YI, ZI), vregs(2, XI, YI, ZI), vregs(2, XI, YI, ZI),
                vregs(2, XI + 1, YI, ZI), vregs(2, XI, YI + 1, ZI), vregs(2, XI, YI, ZI + 1),
                vregs(YI, ZI), pltpu.VMEM((ZI, ny, 128), f32),
                vregs(2, 2, ZI), vregs(4, 2, 2, ZI), pltpu.VMEM((2, 2) + rows, f32), pltpu.VMEM((4, 2, 2) + rows, f32),
                vregs(2, 2, YI), vregs(4, 2, 2, YI),
                vregs(2, ZI), vregs(2, ZI), pltpu.VMEM((2,) + rows, f32), pltpu.VMEM((2,) + rows, f32),
                vregs(2, YI), vregs(2, YI),
                pltpu.VMEM((2, 2, n_dev, 1, 128), f32), pltpu.VMEM((2, 1, 128), f32), pltpu.VMEM((2, 1, 128), f32),
                pltpu.SemaphoreType.DMA((6, 2)), pltpu.SemaphoreType.DMA((2,)),
                pltpu.SemaphoreType.DMA((2, 2)), pltpu.SemaphoreType.DMA((2, 2)),
                pltpu.SemaphoreType.DMA((4, 6)), pltpu.SemaphoreType.DMA((4, 6)),
                pltpu.SemaphoreType.DMA((3,)), pltpu.SemaphoreType.DMA((3,)),
            ],
            compiler_params=pltpu.CompilerParams(collective_id=0, has_side_effects=True, vmem_limit_bytes=67043328),
            name='cg',
        )(*args)
        x_out = pl.pallas_call(
            functools.partial(cell_order, (XI, YI, ZI)),
            out_shape=jax.ShapeDtypeStruct((2, XB, XI, nz, ny), f32),
            in_specs=[hbm], out_specs=hbm,
            scratch_shapes=[
                vregs(2, XI, YI, ZI), pltpu.VMEM((2, XB, XI, nz, ny), f32), pltpu.VMEM((ZI, ny, 128), f32),
                pltpu.SemaphoreType.DMA((2,)), pltpu.SemaphoreType.DMA((2, XI)),
            ],
            compiler_params=pltpu.CompilerParams(vmem_limit_bytes=67043328),
            name='cell_order',
        )(x_out)
        return jnp.swapaxes(x_out.reshape(2, nx, nz, ny), 2, 3), hist

    return jax.shard_map(local_solve, mesh=mesh, in_specs=(field_spec,) * 6, out_specs=(field_spec, P(None, None)), check_vma=False)
```

```python
import functools

import jax
import jax.numpy as jnp
from jax import lax
from jax.experimental import pallas as pl
from jax.experimental.pallas import tpu as pltpu
from jax.sharding import PartitionSpec as P

ITERS = 20
AXES = ('pz', 'py', 'px')
MESH = pl.DeviceIdType.MESH
XB, YB, ZB = 16, 8, 8


def kernel(sizes, dims, s_hbm, b_hbm, x_hbm, kx_hbm, ky_hbm, kz_hbm, xo_hbm, hist_ref,
           stage, r, p, q, x, s, kx, ky, kz, fx, tmp,
           xs, xr, ys, yr, zs, zr, kxs, kxr, kys, kyr, kzs, kzr,
           dots, rho, hist,
           in_sem, out_sem, dot_send, dot_recv, halo_send, halo_recv, k_send, k_recv):
    nz_dev, ny_dev, nx_dev = sizes
    n_dev = nz_dev * ny_dev * nx_dev
    XI, YI, ZI, cells = dims
    pz, py, px = (lax.axis_index(a) for a in AXES)
    me = (pz * ny_dev + py) * nx_dev + px
    lane = lax.broadcasted_iota(jnp.int32, (8, 128), 1)
    sub = lax.broadcasted_iota(jnp.int32, (8, 128), 0)
    lane_z = lax.rem(lane, ZB)
    lane_x = lax.div(lane, ZB)
    row_lane = lax.broadcasted_iota(jnp.int32, (1, 128), 1)

    arrays = (x_hbm, kx_hbm, ky_hbm, kz_hbm, s_hbm, b_hbm)

    def in_copy(a, c):
        return pltpu.make_async_copy(arrays[a].at[c], stage.at[a, c], in_sem.at[a, c])

    for a in range(6):
        for c in range(2):
            in_copy(a, c).start()

    for ref in (xr, yr, zr, kxr, kyr, kzr):
        ref[...] = jnp.zeros(ref.shape, ref.dtype)

    def far_first(pos, size, n):
        high = lax.div(2 * pos, size)
        return high * n + (1 - high) * (size - 1 - n)

    def each_other(fn):
        def step(n, _):
            dev = (far_first(pz, nz_dev, lax.div(n, ny_dev * nx_dev)),
                   far_first(py, ny_dev, lax.rem(lax.div(n, nx_dev), ny_dev)),
                   far_first(px, nx_dev, lax.rem(n, nx_dev)))

            @pl.when((dev[0] * ny_dev + dev[1]) * nx_dev + dev[2] != me)
            def _():
                fn(dev)
            return 0
        lax.fori_loop(0, n_dev, step, 0, unroll=True)

    barrier = pltpu.get_barrier_semaphore()
    each_other(lambda dev: pl.semaphore_signal(barrier, inc=1, device_id=dev, device_id_type=MESH))
    pl.semaphore_wait(barrier, n_dev - 1)

    def unrolled(n, fn):
        def step(i, _):
            fn(i)
            return 0
        lax.fori_loop(0, n, step, 0, unroll=True)

    ysl, zsl = slice(1, YI + 1), slice(1, ZI + 1)
    xsl = slice(1, XI + 1)
    ytail = slice(min(YI, ZB) + 1, YI + 1)

    def relayout(a, stores):
        def system(c, _):
            in_copy(a, c).wait()

            def plane(xi, _):
                def load(zi):
                    rows = stage[a, c, :, xi, pl.ds(zi, ZB, stride=ZI), :]
                    tmp[zi] = rows.reshape(128, rows.shape[-1]).T
                unrolled(ZI, load)
                unrolled(ZI, lambda zi: unrolled(YI, lambda yi: stores(c, xi, yi, zi, tmp[zi, pl.ds(yi, YB, stride=YI), :])))
                return 0
            return lax.fori_loop(0, XI, plane, 0)
        lax.fori_loop(0, 2, system, 0)

    def pack_x(get, shift, put):
        acc = pltpu.roll(get(0), shift, 2) if shift else get(0)
        for j in range(1, YI):
            acc = jnp.where(lane_x == j, pltpu.roll(get(j), (shift + ZB * j) % 128, 2), acc)
        put(acc)

    ycut = min(YI, ZB)

    def pack_z(get, src_zb, put):
        def merge(count, part):
            acc = None
            for j in range(count):
                v = part(j)
                v = pltpu.roll(v, (j - src_zb) % 128, 2) if j != src_zb else v
                acc = v if acc is None else jnp.where(lane_z == j, v, acc)
            return acc
        put(slice(0, XI), merge(ycut, lambda yi: get(slice(0, XI), yi)))
        if YI > ycut:
            put(slice(XI, XI + YI - ycut), merge(XI, lambda xi: get(xi, slice(ycut, YI))))

    def ghost_x(v, packed, j, low):
        dst = 0 if low else XB - 1
        moved = pltpu.roll(v, ZB if low else 128 - ZB, 2)
        move = (ZB * (dst - j)) % 128
        return jnp.where(lane_x == dst, pltpu.roll(packed, move, 2) if move else packed, moved)

    def ghost_z(v, packed, j, low):
        dst = 0 if low else ZB - 1
        moved = pltpu.roll(v, 1 if low else 127, 2)
        move = (dst - j) % 128
        return jnp.where(lane_z == dst, pltpu.roll(packed, move, 2) if move else packed, moved)

    def ghost_y(v, rows, low):
        dst = 0 if low else YB - 1
        moved = pltpu.roll(v, 1 if low else YB - 1, v.ndim - 2)
        return jnp.where(sub == dst, jnp.broadcast_to(rows, v.shape), moved)

    def pack_field(f, c, o):
        def put(ref, d):
            def put_(*v):
                ref[(d, c) + v[:-1]] = v[-1]
            return put_
        xa, za = slice(o, o + XI), slice(o, o + ZI)

        def line(i):
            return slice(i.start + o, i.stop + o) if isinstance(i, slice) else i + o
        pack_x(lambda yi: f[c, o, yi + o, za], 0, put(xs, 0))
        pack_x(lambda yi: f[c, XI - 1 + o, yi + o, za], ZB, put(xs, 1))
        pack_z(lambda xi, yi: f[c, line(xi), line(yi), o], 0, put(zs, 0))
        pack_z(lambda xi, yi: f[c, line(xi), line(yi), ZI - 1 + o], ZB - 1, put(zs, 1))
        ys[0, c] = f[c, xa, o, za, 0:1, :]
        ys[1, c] = f[c, xa, YI - 1 + o, za, YB - 1:YB, :]

    def ghost_field(f, c, w):
        for yi in range(YI):
            f[c, 0, yi + 1, zsl] = ghost_x(f[c, XI, yi + 1, zsl], xr[w, 0, c], yi, True)
            f[c, XI + 1, yi + 1, zsl] = ghost_x(f[c, 1, yi + 1, zsl], xr[w, 1, c], yi, False)
        for yi in range(ycut):
            f[c, xsl, yi + 1, 0] = ghost_z(f[c, xsl, yi + 1, ZI], zr[w, 0, c, :XI], yi, True)
            f[c, xsl, yi + 1, ZI + 1] = ghost_z(f[c, xsl, yi + 1, 1], zr[w, 1, c, :XI], yi, False)
        if YI > ycut:
            for xi in range(XI):
                f[c, xi + 1, ytail, 0] = ghost_z(f[c, xi + 1, ytail, ZI], zr[w, 0, c, XI:], xi, True)
                f[c, xi + 1, ytail, ZI + 1] = ghost_z(f[c, xi + 1, ytail, 1], zr[w, 1, c, XI:], xi, False)
        f[c, xsl, 0, zsl] = ghost_y(f[c, xsl, YI, zsl], yr[w, 0, c], True)
        f[c, xsl, YI + 1, zsl] = ghost_y(f[c, xsl, 1, zsl], yr[w, 1, c], False)

    lower = ((px > 0, (pz, py, px - 1)), (py > 0, (pz, py - 1, px)), (pz > 0, (pz - 1, py, px)))
    upper = ((px < nx_dev - 1, (pz, py, px + 1)), (py < ny_dev - 1, (pz, py + 1, px)), (pz < nz_dev - 1, (pz + 1, py, px)))

    def halo_copies(w):
        out = []
        for axis, (src, dst) in enumerate(((xs, xr), (ys, yr), (zs, zr))):
            for d in range(2):
                ok_send, dev = (lower, upper)[d][axis]
                ok_recv, _ = (upper, lower)[d][axis]
                cp = pltpu.make_async_remote_copy(
                    src_ref=src.at[d], dst_ref=dst.at[w, 1 - d], send_sem=halo_send.at[w, 2 * axis + d],
                    recv_sem=halo_recv.at[w, 2 * axis + d], device_id=dev, device_id_type=MESH)
                out.append((ok_send, ok_recv, cp))
        return out

    def k_copies():
        out = []
        for axis, (src, dst) in enumerate(((kxs, kxr), (kys, kyr), (kzs, kzr))):
            cp = pltpu.make_async_remote_copy(
                src_ref=src, dst_ref=dst, send_sem=k_send.at[axis], recv_sem=k_recv.at[axis],
                device_id=upper[axis][1], device_id_type=MESH)
            out.append((upper[axis][0], lower[axis][0], cp))
        return out

    def start_all(copies):
        for ok_send, _, cp in copies:
            pl.when(ok_send)(cp.start)

    def wait_all(copies):
        for ok_send, ok_recv, cp in copies:
            pl.when(ok_send)(cp.wait_send)
            pl.when(ok_recv)(cp.wait_recv)

    def send_dot(kind, c, acc):
        acc = jnp.sum(acc, axis=0)
        dots[kind, c, me] = jnp.sum(acc, axis=0, keepdims=True)
        each_other(lambda dev: pltpu.make_async_remote_copy(
            src_ref=dots.at[kind, c, me], dst_ref=dots.at[kind, c, me], send_sem=dot_send.at[kind, c],
            recv_sem=dot_recv.at[kind, c], device_id=dev, device_id_type=MESH).start())

    def wait_dot(kind, c):
        rows = dots.at[kind, c, pl.ds(0, n_dev - 1)]
        cp = pltpu.make_async_remote_copy(
            src_ref=rows, dst_ref=rows, send_sem=dot_send.at[kind, c], recv_sem=dot_recv.at[kind, c],
            device_id=(pz, py, px), device_id_type=MESH)
        cp.wait_recv()
        cp.wait_send()
        terms = [dots[kind, c, d] for d in range(n_dev)]
        while len(terms) > 1:
            terms = [terms[i] + terms[i + 1] for i in range(0, len(terms), 2)]
        total = jnp.sum(terms[0], axis=1, keepdims=True)
        return jnp.broadcast_to(total, (1, 128))

    def phase_a(c, beta):
        if beta is not None:
            beta = jnp.broadcast_to(beta, (8, 128))

        def new_p(*idx):
            if beta is not None:
                p[idx] = r[idx] + beta * p[idx]

        def head(yi):
            new_p(c, 0, yi + 1, zsl)
            new_p(c, 1, yi + 1, zsl)
            fx[yi] = kx[c, 0, yi] * (p[c, 0, yi + 1, zsl] - p[c, 1, yi + 1, zsl])
        unrolled(YI, head)

        def plane(xi, acc):
            new_p(c, xi + 1, ysl, 0)
            new_p(c, xi + 1, ysl, ZI + 1)
            new_p(c, xi + 1, 0, zsl)
            new_p(c, xi + 1, YI + 1, zsl)
            pc = p[c, xi + 1, 1, zsl]
            fy_lo = ky[c, xi, 0] * (p[c, xi + 1, 0, zsl] - pc)

            def line(yi, carry):
                acc, pc, fy_lo = carry
                new_p(c, xi + 2, yi + 1, zsl)
                py_hi = p[c, xi + 1, yi + 2, zsl]
                fx_lo = fx[yi]
                fx_hi = kx[c, xi + 1, yi] * (pc - p[c, xi + 2, yi + 1, zsl])
                fx[yi] = fx_hi
                fy_hi = ky[c, xi, yi + 1] * (pc - py_hi)
                fz = kz[c, xi, yi] * (p[c, xi + 1, yi + 1, :ZI + 1] - p[c, xi + 1, yi + 1, 1:])
                out = s[c, xi, yi] * pc + (fx_hi - fx_lo) + (fy_hi - fy_lo) + (fz[1:] - fz[:-1])
                q[c, xi, yi] = out
                return acc + pc * out, py_hi, fy_hi
            return lax.fori_loop(0, YI, line, (acc, pc, fy_lo), unroll=True)[0]
        return lax.fori_loop(0, XI, plane, jnp.zeros((ZI, 8, 128), jnp.float32))

    def phase_b(c, alpha):
        if alpha is not None:
            alpha = jnp.broadcast_to(alpha, (8, 128))

        def plane(xi, acc):
            def line(yi, acc):
                step = q[c, xi, yi] if alpha is None else alpha * q[c, xi, yi]
                v = r[c, xi + 1, yi + 1, zsl] - step
                r[c, xi + 1, yi + 1, zsl] = v
                return acc + v * v
            return lax.fori_loop(0, YI, line, acc, unroll=True)
        return lax.fori_loop(0, XI, plane, jnp.zeros((ZI, 8, 128), jnp.float32))

    def phase_x(c, alpha):
        alpha = jnp.broadcast_to(alpha, (8, 128))

        def plane(xi, _):
            x[c, xi] = x[c, xi] + alpha * p[c, xi + 1, ysl, zsl]
            return 0
        lax.fori_loop(0, XI, plane, 0)

    def both(fn):
        def system(c, _):
            fn(c)
            return 0
        lax.fori_loop(0, 2, system, 0)

    def put_x(c, xi, yi, zi, v):
        p[c, xi + 1, yi + 1, zi + 1] = v
        x[c, xi, yi, zi] = v
    relayout(0, put_x)
    both(lambda c: pack_field(p, c, 1))
    start_all(halo_copies(1))

    def put_to(ref, ox, oy, oz):
        def put(c, xi, yi, zi, v):
            ref[c, xi + ox, yi + oy, zi + oz] = v
        return put
    relayout(1, put_to(kx, 1, 0, 0))
    relayout(2, put_to(ky, 0, 1, 0))
    relayout(3, put_to(kz, 0, 0, 1))

    def pack_k(c):
        def put(ref):
            def put_(*v):
                ref[(c,) + v[:-1]] = v[-1]
            return put_
        pack_x(lambda yi: kx[c, XI, yi], ZB, put(kxs))
        pack_z(lambda xi, yi: kz[c, xi, yi, ZI], ZB - 1, put(kzs))
        kys[c] = ky[c, :, YI, :, YB - 1:YB, :]
    both(pack_k)
    start_all(k_copies())
    relayout(4, put_to(s, 0, 0, 0))
    relayout(5, put_to(r, 1, 1, 1))
    wait_all(halo_copies(1))
    both(lambda c: ghost_field(p, c, 1))
    wait_all(k_copies())

    def ghost_k(c):
        def edge(cond, v):
            return jnp.where(cond, 0.0, v)
        for yi in range(YI):
            v = kx[c, XI, yi]
            kx[c, 0, yi] = ghost_x(v, kxr[c], yi, True)
            kx[c, XI, yi] = edge(jnp.logical_and(lane_x == XB - 1, px == nx_dev - 1), v)
        for yi in range(ycut):
            kz[c, :, yi, 0] = ghost_z(kz[c, :, yi, ZI], kzr[c, :XI], yi, True)
        if YI > ycut:
            for xi in range(XI):
                kz[c, xi, ycut:, 0] = ghost_z(kz[c, xi, ycut:, ZI], kzr[c, XI:], xi, True)
        kz[c, :, :, ZI] = edge(jnp.logical_and(lane_z == ZB - 1, pz == nz_dev - 1), kz[c, :, :, ZI])
        v = ky[c, :, YI]
        ky[c, :, 0] = ghost_y(v, kyr[c], True)
        ky[c, :, YI] = edge(jnp.logical_and(sub == YB - 1, py == ny_dev - 1), v)
    both(ghost_k)

    for c in range(2):
        phase_a(c, None)
        send_dot(1, c, phase_b(c, None))
    both(lambda c: pack_field(r, c, 1))
    start_all(halo_copies(0))
    rho[...] = jnp.ones(rho.shape, jnp.float32)
    hist[...] = jnp.zeros(hist.shape, jnp.float32)
    wait_all(halo_copies(0))
    both(lambda c: ghost_field(r, c, 0))

    def new_rho(c, k):
        total = wait_dot(1, c)
        ratio = total / rho[c]
        rho[c] = total
        hist[c] = jnp.where(row_lane == k, total, hist[c])
        return ratio

    def iteration(k, _):
        slot = 2 + lax.rem(k, 2)
        for c in range(2):
            beta = new_rho(c, k)
            beta = jnp.where(k == 0, 0.0, beta)
            send_dot(0, c, phase_a(c, beta))

        @pl.when(k < ITERS - 1)
        def _():
            both(lambda c: pack_field(q, c, 0))
            start_all(halo_copies(slot))
        alphas = []
        for c in range(2):
            alpha = rho[c] / wait_dot(0, c)
            alphas.append(alpha)
            send_dot(1, c, phase_b(c, alpha))
        for c in range(2):
            phase_x(c, alphas[c])

        @pl.when(k < ITERS - 1)
        def _():
            wait_all(halo_copies(slot))
            for ref in (xr, yr, zr):
                for d in range(2):
                    for c in range(2):
                        ref[0, d, c] = ref[0, d, c] - alphas[c] * ref[slot, d, c]
            both(lambda c: ghost_field(r, c, 0))
        return 0
    lax.fori_loop(0, ITERS, iteration, 0)

    for c in range(2):
        pltpu.make_async_copy(x.at[c], xo_hbm.at[c], out_sem.at[c]).start()
    for c in range(2):
        new_rho(c, ITERS)
        hist_ref[c:c + 1, :] = jnp.sqrt(hist[c] / cells)[:, :ITERS + 1]
    for c in range(2):
        pltpu.make_async_copy(x.at[c], xo_hbm.at[c], out_sem.at[c]).wait()


def cell_order(dims, x_hbm, hist_in, o_hbm, hist_out, x, stage, tmp, in_sem, out_sem):
    XI, YI, ZI = dims

    def in_copy(c, xi):
        return pltpu.make_async_copy(x_hbm.at[c, xi], x.at[c, xi], in_sem.at[c, xi])

    def out_copy(c, xi):
        return pltpu.make_async_copy(stage.at[c, :, xi], o_hbm.at[c, :, xi], out_sem.at[c, xi])

    for c in range(2):
        for xi in range(XI):
            in_copy(c, xi).start()
    hist_out[...] = hist_in[...]
    for c in range(2):
        def plane(xi, _):
            in_copy(c, xi).wait()
            for zi in range(ZI):
                for yi in range(YI):
                    tmp[zi, pl.ds(yi, YB, stride=YI), :] = x[c, xi, yi, zi]
            for zi in range(ZI):
                stage[c, :, xi, pl.ds(zi, ZB, stride=ZI), :] = tmp[zi].T.reshape(XB, ZB, tmp.shape[1])
            out_copy(c, xi).start()
            return 0
        lax.fori_loop(0, XI, plane, 0)
    for c in range(2):
        for xi in range(XI):
            out_copy(c, xi).wait()


def solution(mesh):
    sizes = tuple(mesh.shape[a] for a in AXES)
    n_dev = sizes[0] * sizes[1] * sizes[2]
    field_spec = P(None, 'px', 'py', 'pz')

    def local_solve(*args):
        _, nx, ny, nz = args[0].shape
        XI, YI, ZI = nx // XB, ny // YB, nz // ZB
        cells = float(nx * ny * nz * n_dev)
        f32 = jnp.float32
        rows = (XI, ZI, 1, 128)
        mz = XI + max(0, YI - ZB)

        def vregs(*lead):
            return pltpu.VMEM(lead + (8, 128), f32)
        hbm = pl.BlockSpec(memory_space=pl.ANY)
        args = [jnp.swapaxes(a, 2, 3).reshape(2, XB, XI, nz, ny) for a in args]
        x_out, hist = pl.pallas_call(
            functools.partial(kernel, sizes, (XI, YI, ZI, cells)),
            out_shape=(jax.ShapeDtypeStruct((2, XI, YI, ZI, 8, 128), f32), jax.ShapeDtypeStruct((2, ITERS + 1), f32)),
            in_specs=[hbm] * 6,
            out_specs=(hbm, pl.BlockSpec(memory_space=pltpu.VMEM)),
            scratch_shapes=[
                pltpu.VMEM((6, 2, XB, XI, nz, ny), f32),
                vregs(2, XI + 2, YI + 2, ZI + 2), vregs(2, XI + 2, YI + 2, ZI + 2),
                vregs(2, XI, YI, ZI), vregs(2, XI, YI, ZI), vregs(2, XI, YI, ZI),
                vregs(2, XI + 1, YI, ZI), vregs(2, XI, YI + 1, ZI), vregs(2, XI, YI, ZI + 1),
                vregs(YI, ZI), pltpu.VMEM((ZI, ny, 128), f32),
                vregs(2, 2, ZI), vregs(4, 2, 2, ZI), pltpu.VMEM((2, 2) + rows, f32), pltpu.VMEM((4, 2, 2) + rows, f32),
                vregs(2, 2, mz), vregs(4, 2, 2, mz),
                vregs(2, ZI), vregs(2, ZI), pltpu.VMEM((2,) + rows, f32), pltpu.VMEM((2,) + rows, f32),
                vregs(2, mz), vregs(2, mz),
                pltpu.VMEM((2, 2, n_dev, 1, 128), f32), pltpu.VMEM((2, 1, 128), f32), pltpu.VMEM((2, 1, 128), f32),
                pltpu.SemaphoreType.DMA((6, 2)), pltpu.SemaphoreType.DMA((2,)),
                pltpu.SemaphoreType.DMA((2, 2)), pltpu.SemaphoreType.DMA((2, 2)),
                pltpu.SemaphoreType.DMA((4, 6)), pltpu.SemaphoreType.DMA((4, 6)),
                pltpu.SemaphoreType.DMA((3,)), pltpu.SemaphoreType.DMA((3,)),
            ],
            compiler_params=pltpu.CompilerParams(collective_id=0, has_side_effects=True, vmem_limit_bytes=67043328),
            name='cg',
        )(*args)
        small = pl.BlockSpec(memory_space=pltpu.VMEM)
        x_out, hist = pl.pallas_call(
            functools.partial(cell_order, (XI, YI, ZI)),
            out_shape=(jax.ShapeDtypeStruct((2, XB, XI, nz, ny), f32), jax.ShapeDtypeStruct(hist.shape, f32)),
            in_specs=[hbm, small], out_specs=(hbm, small),
            scratch_shapes=[
                vregs(2, XI, YI, ZI), pltpu.VMEM((2, XB, XI, nz, ny), f32), pltpu.VMEM((ZI, ny, 128), f32),
                pltpu.SemaphoreType.DMA((2, XI)), pltpu.SemaphoreType.DMA((2, XI)),
            ],
            compiler_params=pltpu.CompilerParams(vmem_limit_bytes=67043328),
            name='cell_order',
        )(x_out, hist)
        return jnp.swapaxes(x_out.reshape(2, nx, nz, ny), 2, 3), hist

    return jax.shard_map(local_solve, mesh=mesh, in_specs=(field_spec,) * 6, out_specs=(field_spec, P(None, None)), check_vma=False)
```

```python
import functools

import jax
import jax.numpy as jnp
from jax import lax
from jax.experimental import pallas as pl
from jax.experimental.pallas import tpu as pltpu
from jax.sharding import PartitionSpec as P

ITERS = 20
AXES = ('pz', 'py', 'px')
MESH = pl.DeviceIdType.MESH
XB, YB, ZB = 16, 8, 8


def kernel(sizes, dims, s_hbm, b_hbm, x_hbm, kx_hbm, ky_hbm, kz_hbm, xo_hbm, hist_ref,
           stage, r, p, q, x, s, kx, ky, kz, tmp,
           xs, xr, ys, yr, zs, zr, kxs, kxr, kys, kyr, kzs, kzr,
           dots, rho, hist,
           in_sem, out_sem, dot_send, dot_recv, halo_send, halo_recv, k_send, k_recv):
    nz_dev, ny_dev, nx_dev = sizes
    n_dev = nz_dev * ny_dev * nx_dev
    XI, YI, ZI, cells = dims
    pz, py, px = (lax.axis_index(a) for a in AXES)
    me = (pz * ny_dev + py) * nx_dev + px
    lane = lax.broadcasted_iota(jnp.int32, (8, 128), 1)
    sub = lax.broadcasted_iota(jnp.int32, (8, 128), 0)
    lane_z = lax.rem(lane, ZB)
    lane_x = lax.div(lane, ZB)
    row_lane = lax.broadcasted_iota(jnp.int32, (1, 128), 1)

    arrays = (x_hbm, kx_hbm, ky_hbm, kz_hbm, s_hbm, b_hbm)

    def in_copy(a, c):
        return pltpu.make_async_copy(arrays[a].at[c], stage.at[a, c], in_sem.at[a, c])

    for a in range(6):
        for c in range(2):
            in_copy(a, c).start()

    for ref in (xr, yr, zr, kxr, kyr, kzr):
        ref[...] = jnp.zeros(ref.shape, ref.dtype)

    def far_first(pos, size, n):
        high = lax.div(2 * pos, size)
        return high * n + (1 - high) * (size - 1 - n)

    def each_other(fn):
        def step(n, _):
            dev = (far_first(pz, nz_dev, lax.div(n, ny_dev * nx_dev)),
                   far_first(py, ny_dev, lax.rem(lax.div(n, nx_dev), ny_dev)),
                   far_first(px, nx_dev, lax.rem(n, nx_dev)))

            @pl.when((dev[0] * ny_dev + dev[1]) * nx_dev + dev[2] != me)
            def _():
                fn(dev)
            return 0
        lax.fori_loop(0, n_dev, step, 0, unroll=True)

    barrier = pltpu.get_barrier_semaphore()
    each_other(lambda dev: pl.semaphore_signal(barrier, inc=1, device_id=dev, device_id_type=MESH))

    def unrolled(n, fn):
        def step(i, _):
            fn(i)
            return 0
        lax.fori_loop(0, n, step, 0, unroll=True)

    ysl, zsl = slice(1, YI + 1), slice(1, ZI + 1)
    xsl = slice(1, XI + 1)
    ytail = slice(min(YI, ZB) + 1, YI + 1)

    def relayout(a, stores):
        def system(c, _):
            in_copy(a, c).wait()

            def plane(xi, _):
                def load(zi):
                    rows = stage[a, c, :, xi, pl.ds(zi, ZB, stride=ZI), :]
                    tmp[zi] = rows.reshape(128, rows.shape[-1]).T
                unrolled(ZI, load)
                unrolled(ZI, lambda zi: unrolled(YI, lambda yi: stores(c, xi, yi, zi, tmp[zi, pl.ds(yi, YB, stride=YI), :])))
                return 0
            return lax.fori_loop(0, XI, plane, 0)
        lax.fori_loop(0, 2, system, 0)

    def pack_x(get, shift, put):
        acc = pltpu.roll(get(0), shift, 2) if shift else get(0)
        for j in range(1, YI):
            acc = jnp.where(lane_x == j, pltpu.roll(get(j), (shift + ZB * j) % 128, 2), acc)
        put(acc)

    ycut = min(YI, ZB)

    def pack_z(get, src_zb, put):
        def merge(count, part):
            acc = None
            for j in range(count):
                v = part(j)
                v = pltpu.roll(v, (j - src_zb) % 128, 2) if j != src_zb else v
                acc = v if acc is None else jnp.where(lane_z == j, v, acc)
            return acc
        put(slice(0, XI), merge(ycut, lambda yi: get(slice(0, XI), yi)))
        if YI > ycut:
            put(slice(XI, XI + YI - ycut), merge(XI, lambda xi: get(xi, slice(ycut, YI))))

    def ghost_x(v, packed, j, low):
        dst = 0 if low else XB - 1
        moved = pltpu.roll(v, ZB if low else 128 - ZB, 2)
        move = (ZB * (dst - j)) % 128
        return jnp.where(lane_x == dst, pltpu.roll(packed, move, 2) if move else packed, moved)

    def ghost_z(v, packed, j, low):
        dst = 0 if low else ZB - 1
        moved = pltpu.roll(v, 1 if low else 127, 2)
        move = (dst - j) % 128
        return jnp.where(lane_z == dst, pltpu.roll(packed, move, 2) if move else packed, moved)

    def ghost_y(v, rows, low):
        dst = 0 if low else YB - 1
        moved = pltpu.roll(v, 1 if low else YB - 1, v.ndim - 2)
        return jnp.where(sub == dst, jnp.broadcast_to(rows, v.shape), moved)

    def pack_field(f, c, o):
        def put(ref, d):
            def put_(*v):
                ref[(d, c) + v[:-1]] = v[-1]
            return put_
        xa, za = slice(o, o + XI), slice(o, o + ZI)

        def line(i):
            return slice(i.start + o, i.stop + o) if isinstance(i, slice) else i + o
        pack_x(lambda yi: f[c, o, yi + o, za], 0, put(xs, 0))
        pack_x(lambda yi: f[c, XI - 1 + o, yi + o, za], ZB, put(xs, 1))
        pack_z(lambda xi, yi: f[c, line(xi), line(yi), o], 0, put(zs, 0))
        pack_z(lambda xi, yi: f[c, line(xi), line(yi), ZI - 1 + o], ZB - 1, put(zs, 1))
        ys[0, c] = f[c, xa, o, za, 0:1, :]
        ys[1, c] = f[c, xa, YI - 1 + o, za, YB - 1:YB, :]

    def ghost_field(f, c, w):
        for yi in range(YI):
            f[c, 0, yi + 1, zsl] = ghost_x(f[c, XI, yi + 1, zsl], xr[w, 0, c], yi, True)
            f[c, XI + 1, yi + 1, zsl] = ghost_x(f[c, 1, yi + 1, zsl], xr[w, 1, c], yi, False)
        for yi in range(ycut):
            f[c, xsl, yi + 1, 0] = ghost_z(f[c, xsl, yi + 1, ZI], zr[w, 0, c, :XI], yi, True)
            f[c, xsl, yi + 1, ZI + 1] = ghost_z(f[c, xsl, yi + 1, 1], zr[w, 1, c, :XI], yi, False)
        if YI > ycut:
            for xi in range(XI):
                f[c, xi + 1, ytail, 0] = ghost_z(f[c, xi + 1, ytail, ZI], zr[w, 0, c, XI:], xi, True)
                f[c, xi + 1, ytail, ZI + 1] = ghost_z(f[c, xi + 1, ytail, 1], zr[w, 1, c, XI:], xi, False)
        f[c, xsl, 0, zsl] = ghost_y(f[c, xsl, YI, zsl], yr[w, 0, c], True)
        f[c, xsl, YI + 1, zsl] = ghost_y(f[c, xsl, 1, zsl], yr[w, 1, c], False)

    lower = ((px > 0, (pz, py, px - 1)), (py > 0, (pz, py - 1, px)), (pz > 0, (pz - 1, py, px)))
    upper = ((px < nx_dev - 1, (pz, py, px + 1)), (py < ny_dev - 1, (pz, py + 1, px)), (pz < nz_dev - 1, (pz + 1, py, px)))

    def halo_copies(w):
        out = []
        for axis, (src, dst) in enumerate(((xs, xr), (ys, yr), (zs, zr))):
            for d in range(2):
                ok_send, dev = (lower, upper)[d][axis]
                ok_recv, _ = (upper, lower)[d][axis]
                cp = pltpu.make_async_remote_copy(
                    src_ref=src.at[d], dst_ref=dst.at[w, 1 - d], send_sem=halo_send.at[w, 2 * axis + d],
                    recv_sem=halo_recv.at[w, 2 * axis + d], device_id=dev, device_id_type=MESH)
                out.append((ok_send, ok_recv, cp))
        return out

    def k_copies():
        out = []
        for axis, (src, dst) in enumerate(((kxs, kxr), (kys, kyr), (kzs, kzr))):
            cp = pltpu.make_async_remote_copy(
                src_ref=src, dst_ref=dst, send_sem=k_send.at[axis], recv_sem=k_recv.at[axis],
                device_id=upper[axis][1], device_id_type=MESH)
            out.append((upper[axis][0], lower[axis][0], cp))
        return out

    def start_all(copies):
        for ok_send, _, cp in copies:
            pl.when(ok_send)(cp.start)

    def wait_all(copies):
        for ok_send, ok_recv, cp in copies:
            pl.when(ok_send)(cp.wait_send)
            pl.when(ok_recv)(cp.wait_recv)

    def send_dot(kind, c, acc):
        acc = jnp.sum(acc, axis=0)
        dots[kind, c, me] = jnp.sum(acc, axis=0, keepdims=True)
        each_other(lambda dev: pltpu.make_async_remote_copy(
            src_ref=dots.at[kind, c, me], dst_ref=dots.at[kind, c, me], send_sem=dot_send.at[kind, c],
            recv_sem=dot_recv.at[kind, c], device_id=dev, device_id_type=MESH).start())

    def wait_dot(kind, c):
        rows = dots.at[kind, c, pl.ds(0, n_dev - 1)]
        cp = pltpu.make_async_remote_copy(
            src_ref=rows, dst_ref=rows, send_sem=dot_send.at[kind, c], recv_sem=dot_recv.at[kind, c],
            device_id=(pz, py, px), device_id_type=MESH)
        cp.wait_recv()
        cp.wait_send()
        terms = [dots[kind, c, d] for d in range(n_dev)]
        while len(terms) > 1:
            terms = [terms[i] + terms[i + 1] for i in range(0, len(terms), 2)]
        total = jnp.sum(terms[0], axis=1, keepdims=True)
        return jnp.broadcast_to(total, (1, 128))

    def phase_a(c, beta):
        if beta is not None:
            beta = jnp.broadcast_to(beta, (8, 128))

        def new_p(*idx):
            if beta is not None:
                p[idx] = r[idx] + beta * p[idx]

        def head(yi):
            new_p(c, 0, yi + 1, zsl)
            new_p(c, 1, yi + 1, zsl)
        unrolled(YI, head)

        def plane(xi, acc):
            new_p(c, xi + 1, ysl, 0)
            new_p(c, xi + 1, ysl, ZI + 1)
            new_p(c, xi + 1, 0, zsl)
            new_p(c, xi + 1, YI + 1, zsl)

            def line(yi, carry):
                acc, py_lo, pc, ky_lo = carry
                new_p(c, xi + 2, yi + 1, zsl)
                py_hi = p[c, xi + 1, yi + 2, zsl]
                ky_hi = ky[c, xi, yi + 1]
                out = s[c, xi, yi] * pc - ky_lo * py_lo - ky_hi * py_hi
                out = out - kx[c, xi, yi] * p[c, xi, yi + 1, zsl]
                out = out - kz[c, xi, yi, :ZI] * p[c, xi + 1, yi + 1, :ZI]
                out = out - kz[c, xi, yi, 1:] * p[c, xi + 1, yi + 1, 2:]
                out = out - kx[c, xi + 1, yi] * p[c, xi + 2, yi + 1, zsl]
                q[c, xi, yi] = out
                return acc + pc * out, pc, py_hi, ky_hi
            carry = (acc, p[c, xi + 1, 0, zsl], p[c, xi + 1, 1, zsl], ky[c, xi, 0])
            return lax.fori_loop(0, YI, line, carry, unroll=True)[0]
        return lax.fori_loop(0, XI, plane, jnp.zeros((ZI, 8, 128), jnp.float32))

    def phase_b(c, alpha):
        if alpha is not None:
            alpha = jnp.broadcast_to(alpha, (8, 128))

        def plane(xi, acc):
            def line(yi, acc):
                step = q[c, xi, yi] if alpha is None else alpha * q[c, xi, yi]
                v = r[c, xi + 1, yi + 1, zsl] - step
                r[c, xi + 1, yi + 1, zsl] = v
                return acc + v * v
            return lax.fori_loop(0, YI, line, acc, unroll=True)
        return lax.fori_loop(0, XI, plane, jnp.zeros((ZI, 8, 128), jnp.float32))

    def phase_x(c, alpha):
        alpha = jnp.broadcast_to(alpha, (8, 128))

        def plane(xi, _):
            x[c, xi] = x[c, xi] + alpha * p[c, xi + 1, ysl, zsl]
            return 0
        lax.fori_loop(0, XI, plane, 0)

    def both(fn):
        def system(c, _):
            fn(c)
            return 0
        lax.fori_loop(0, 2, system, 0)

    def put_x(c, xi, yi, zi, v):
        p[c, xi + 1, yi + 1, zi + 1] = v
        x[c, xi, yi, zi] = v
    relayout(0, put_x)
    both(lambda c: pack_field(p, c, 1))

    def put_to(ref, ox, oy, oz):
        def put(c, xi, yi, zi, v):
            ref[c, xi + ox, yi + oy, zi + oz] = v
        return put

    def put_k(ref, c):
        def put_(*v):
            ref[(c,) + v[:-1]] = v[-1]
        return put_

    def edge(cond, v):
        return jnp.where(cond, 0.0, v)
    copies_x, copies_y, copies_z = k_copies()
    relayout(3, put_to(kz, 0, 0, 1))
    both(lambda c: pack_z(lambda xi, yi: kz[c, xi, yi, ZI], ZB - 1, put_k(kzs, c)))
    pl.semaphore_wait(barrier, n_dev - 1)
    start_all(halo_copies(1))
    start_all([copies_z])
    relayout(1, put_to(kx, 1, 0, 0))
    both(lambda c: pack_x(lambda yi: kx[c, XI, yi], ZB, put_k(kxs, c)))
    start_all([copies_x])
    relayout(2, put_to(ky, 0, 1, 0))
    for c in range(2):
        kys[c] = ky[c, :, YI, :, YB - 1:YB, :]
    start_all([copies_y])
    relayout(4, put_to(s, 0, 0, 0))
    relayout(5, put_to(r, 1, 1, 1))
    wait_all(halo_copies(1))
    both(lambda c: ghost_field(p, c, 1))
    wait_all([copies_z, copies_x, copies_y])

    def ghost_k(c):
        for yi in range(YI):
            v = kx[c, XI, yi]
            kx[c, 0, yi] = ghost_x(v, kxr[c], yi, True)
            kx[c, XI, yi] = edge(jnp.logical_and(lane_x == XB - 1, px == nx_dev - 1), v)
        for yi in range(ycut):
            kz[c, :, yi, 0] = ghost_z(kz[c, :, yi, ZI], kzr[c, :XI], yi, True)
        if YI > ycut:
            for xi in range(XI):
                kz[c, xi, ycut:, 0] = ghost_z(kz[c, xi, ycut:, ZI], kzr[c, XI:], xi, True)
        kz[c, :, :, ZI] = edge(jnp.logical_and(lane_z == ZB - 1, pz == nz_dev - 1), kz[c, :, :, ZI])
        v = ky[c, :, YI]
        ky[c, :, 0] = ghost_y(v, kyr[c], True)
        ky[c, :, YI] = edge(jnp.logical_and(sub == YB - 1, py == ny_dev - 1), v)

        def diagonal(xi, _):
            def line(yi):
                v = s[c, xi, yi] + (kx[c, xi, yi] + kx[c, xi + 1, yi]) + (ky[c, xi, yi] + ky[c, xi, yi + 1])
                s[c, xi, yi] = v + (kz[c, xi, yi, :ZI] + kz[c, xi, yi, 1:])
            unrolled(YI, line)
            return 0
        lax.fori_loop(0, XI, diagonal, 0)
    both(ghost_k)

    for c in range(2):
        phase_a(c, None)
        send_dot(1, c, phase_b(c, None))
    both(lambda c: pack_field(r, c, 1))
    start_all(halo_copies(0))
    rho[...] = jnp.ones(rho.shape, jnp.float32)
    hist[...] = jnp.zeros(hist.shape, jnp.float32)
    wait_all(halo_copies(0))
    both(lambda c: ghost_field(r, c, 0))

    def new_rho(c, k):
        total = wait_dot(1, c)
        ratio = total / rho[c]
        rho[c] = total
        hist[c] = jnp.where(row_lane == k, total, hist[c])
        return ratio

    def iteration(k, _):
        slot = 2 + lax.rem(k, 2)
        for c in range(2):
            beta = new_rho(c, k)
            beta = jnp.where(k == 0, 0.0, beta)
            send_dot(0, c, phase_a(c, beta))

        @pl.when(k < ITERS - 1)
        def _():
            both(lambda c: pack_field(q, c, 0))
            start_all(halo_copies(slot))
        alphas = []
        for c in range(2):
            alpha = rho[c] / wait_dot(0, c)
            alphas.append(alpha)
            send_dot(1, c, phase_b(c, alpha))
        for c in range(2):
            phase_x(c, alphas[c])

        @pl.when(k < ITERS - 1)
        def _():
            wait_all(halo_copies(slot))
            for ref in (xr, yr, zr):
                for d in range(2):
                    for c in range(2):
                        ref[0, d, c] = ref[0, d, c] - alphas[c] * ref[slot, d, c]
            both(lambda c: ghost_field(r, c, 0))
        return 0
    lax.fori_loop(0, ITERS, iteration, 0)

    for c in range(2):
        pltpu.make_async_copy(x.at[c], xo_hbm.at[c], out_sem.at[c]).start()
    for c in range(2):
        new_rho(c, ITERS)
        hist_ref[c:c + 1, :] = jnp.sqrt(hist[c] / cells)[:, :ITERS + 1]
    for c in range(2):
        pltpu.make_async_copy(x.at[c], xo_hbm.at[c], out_sem.at[c]).wait()


def cell_order(dims, x_hbm, hist_in, o_hbm, hist_out, x, stage, tmp, hist, in_sem, out_sem, hist_sem):
    XI, YI, ZI = dims

    def in_copy(c, xi):
        return pltpu.make_async_copy(x_hbm.at[c, xi], x.at[c, xi], in_sem.at[c, xi])

    def out_copy(c, xi):
        return pltpu.make_async_copy(stage.at[c, :, xi], o_hbm.at[c, :, xi], out_sem.at[c, xi])
    hist_copies = pltpu.make_async_copy(hist_in, hist, hist_sem.at[0]), pltpu.make_async_copy(hist, hist_out, hist_sem.at[1])

    for c in range(2):
        for xi in range(XI):
            in_copy(c, xi).start()
    hist_copies[0].start()
    for c in range(2):
        def plane(xi, _):
            in_copy(c, xi).wait()
            for zi in range(ZI):
                for yi in range(YI):
                    tmp[zi, pl.ds(yi, YB, stride=YI), :] = x[c, xi, yi, zi]
            for zi in range(ZI):
                stage[c, :, xi, pl.ds(zi, ZB, stride=ZI), :] = tmp[zi].T.reshape(XB, ZB, tmp.shape[1])
            out_copy(c, xi).start()
            return 0
        lax.fori_loop(0, XI, plane, 0)
        if c == 0:
            hist_copies[0].wait()
            hist_copies[1].start()
    for c in range(2):
        for xi in range(XI):
            out_copy(c, xi).wait()
    hist_copies[1].wait()


def solution(mesh):
    sizes = tuple(mesh.shape[a] for a in AXES)
    n_dev = sizes[0] * sizes[1] * sizes[2]
    field_spec = P(None, 'px', 'py', 'pz')

    def local_solve(*args):
        _, nx, ny, nz = args[0].shape
        XI, YI, ZI = nx // XB, ny // YB, nz // ZB
        cells = float(nx * ny * nz * n_dev)
        f32 = jnp.float32
        rows = (XI, ZI, 1, 128)
        mz = XI + max(0, YI - ZB)

        def vregs(*lead):
            return pltpu.VMEM(lead + (8, 128), f32)
        hbm = pl.BlockSpec(memory_space=pl.ANY)
        args = [jnp.swapaxes(a, 2, 3).reshape(2, XB, XI, nz, ny) for a in args]
        x_out, hist = pl.pallas_call(
            functools.partial(kernel, sizes, (XI, YI, ZI, cells)),
            out_shape=(jax.ShapeDtypeStruct((2, XI, YI, ZI, 8, 128), f32), jax.ShapeDtypeStruct((2, ITERS + 1), f32)),
            in_specs=[hbm] * 6,
            out_specs=(hbm, pl.BlockSpec(memory_space=pltpu.VMEM)),
            scratch_shapes=[
                pltpu.VMEM((6, 2, XB, XI, nz, ny), f32),
                vregs(2, XI + 2, YI + 2, ZI + 2), vregs(2, XI + 2, YI + 2, ZI + 2),
                vregs(2, XI, YI, ZI), vregs(2, XI, YI, ZI), vregs(2, XI, YI, ZI),
                vregs(2, XI + 1, YI, ZI), vregs(2, XI, YI + 1, ZI), vregs(2, XI, YI, ZI + 1),
                pltpu.VMEM((ZI, ny, 128), f32),
                vregs(2, 2, ZI), vregs(4, 2, 2, ZI), pltpu.VMEM((2, 2) + rows, f32), pltpu.VMEM((4, 2, 2) + rows, f32),
                vregs(2, 2, mz), vregs(4, 2, 2, mz),
                vregs(2, ZI), vregs(2, ZI), pltpu.VMEM((2,) + rows, f32), pltpu.VMEM((2,) + rows, f32),
                vregs(2, mz), vregs(2, mz),
                pltpu.VMEM((2, 2, n_dev, 1, 128), f32), pltpu.VMEM((2, 1, 128), f32), pltpu.VMEM((2, 1, 128), f32),
                pltpu.SemaphoreType.DMA((6, 2)), pltpu.SemaphoreType.DMA((2,)),
                pltpu.SemaphoreType.DMA((2, 2)), pltpu.SemaphoreType.DMA((2, 2)),
                pltpu.SemaphoreType.DMA((4, 6)), pltpu.SemaphoreType.DMA((4, 6)),
                pltpu.SemaphoreType.DMA((3,)), pltpu.SemaphoreType.DMA((3,)),
            ],
            compiler_params=pltpu.CompilerParams(collective_id=0, has_side_effects=True, vmem_limit_bytes=67043328),
            name='cg',
        )(*args)
        x_out, hist = pl.pallas_call(
            functools.partial(cell_order, (XI, YI, ZI)),
            out_shape=(jax.ShapeDtypeStruct((2, XB, XI, nz, ny), f32), jax.ShapeDtypeStruct(hist.shape, f32)),
            in_specs=[hbm, hbm], out_specs=(hbm, hbm),
            scratch_shapes=[
                vregs(2, XI, YI, ZI), pltpu.VMEM((2, XB, XI, nz, ny), f32), pltpu.VMEM((ZI, ny, 128), f32),
                pltpu.VMEM(hist.shape, f32),
                pltpu.SemaphoreType.DMA((2, XI)), pltpu.SemaphoreType.DMA((2, XI)), pltpu.SemaphoreType.DMA((2,)),
            ],
            compiler_params=pltpu.CompilerParams(vmem_limit_bytes=67043328),
            name='cell_order',
        )(x_out, hist)
        return jnp.swapaxes(x_out.reshape(2, nx, nz, ny), 2, 3), hist

    return jax.shard_map(local_solve, mesh=mesh, in_specs=(field_spec,) * 6, out_specs=(field_spec, P(None, None)), check_vma=False)
```

```python
import functools

import jax
import jax.numpy as jnp
from jax import lax
from jax.experimental import pallas as pl
from jax.experimental.pallas import tpu as pltpu
from jax.sharding import PartitionSpec as P

ITERS = 20
AXES = ('pz', 'py', 'px')
MESH = pl.DeviceIdType.MESH
XB, YB, ZB = 16, 8, 8


def kernel(sizes, dims, s_hbm, b_hbm, x_hbm, kx_hbm, ky_hbm, kz_hbm, xo_hbm, hist_ref,
           stage, r, p, q, x, s, kx, ky, kz, tmp,
           xs, xr, ys, yr, zs, zr, kxs, kxr, kys, kyr, kzs, kzr,
           dots, rho, hist,
           in_sem, out_sem, dot_send, dot_recv, halo_send, halo_recv, k_send, k_recv):
    nz_dev, ny_dev, nx_dev = sizes
    n_dev = nz_dev * ny_dev * nx_dev
    XI, YI, ZI, cells = dims
    pz, py, px = (lax.axis_index(a) for a in AXES)
    me = (pz * ny_dev + py) * nx_dev + px
    lane = lax.broadcasted_iota(jnp.int32, (8, 128), 1)
    sub = lax.broadcasted_iota(jnp.int32, (8, 128), 0)
    lane_z = lax.rem(lane, ZB)
    lane_x = lax.div(lane, ZB)
    row_lane = lax.broadcasted_iota(jnp.int32, (1, 128), 1)

    arrays = (x_hbm, kx_hbm, ky_hbm, kz_hbm, s_hbm, b_hbm)

    def in_copy(a, c):
        return pltpu.make_async_copy(arrays[a].at[c], stage.at[a, c], in_sem.at[a, c])

    for a in range(6):
        for c in range(2):
            in_copy(a, c).start()

    for ref in (xr, yr, zr, kxr, kyr, kzr):
        ref[...] = jnp.zeros(ref.shape, ref.dtype)

    def far_first(pos, size, n):
        high = lax.div(2 * pos, size)
        return high * n + (1 - high) * (size - 1 - n)

    others = []
    for n in range(n_dev):
        dev = (far_first(pz, nz_dev, n // (ny_dev * nx_dev)), far_first(py, ny_dev, n // nx_dev % ny_dev),
               far_first(lax.div(px, 2), nx_dev // 2, n % nx_dev // 2) * 2 + n % 2)
        others.append((dev, (dev[0] * ny_dev + dev[1]) * nx_dev + dev[2] != me))

    def each_other(fn):
        for dev, is_other in others:
            pl.when(is_other)(functools.partial(fn, dev))

    barrier = pltpu.get_barrier_semaphore()
    each_other(lambda dev: pl.semaphore_signal(barrier, inc=1, device_id=dev, device_id_type=MESH))

    def unrolled(n, fn):
        def step(i, _):
            fn(i)
            return 0
        lax.fori_loop(0, n, step, 0, unroll=True)

    ysl, zsl = slice(1, YI + 1), slice(1, ZI + 1)
    xsl = slice(1, XI + 1)
    ytail = slice(min(YI, ZB) + 1, YI + 1)

    def block(half, i):
        n = half * (XI * ZI // 2) + i
        return lax.div(n, ZI), lax.rem(n, ZI)

    def relayout(a, stores):
        def system(c, _):
            in_copy(a, c).wait()

            def chunk(half, _):
                def load(i):
                    xi, zi = block(half, i)
                    rows = stage[a, c, :, xi, pl.ds(zi, ZB, stride=ZI), :]
                    tmp[i] = rows.reshape(128, rows.shape[-1]).T

                def store(i):
                    xi, zi = block(half, i)
                    unrolled(YI, lambda yi: stores(c, xi, yi, zi, tmp[i, pl.ds(yi, YB, stride=YI), :]))
                unrolled(XI * ZI // 2, load)
                unrolled(XI * ZI // 2, store)
                return 0
            return lax.fori_loop(0, 2, chunk, 0)
        lax.fori_loop(0, 2, system, 0)

    def pack_x(get, shift, put):
        acc = pltpu.roll(get(0), shift, 2) if shift else get(0)
        for j in range(1, YI):
            acc = jnp.where(lane_x == j, pltpu.roll(get(j), (shift + ZB * j) % 128, 2), acc)
        put(acc)

    ycut = min(YI, ZB)

    def pack_z(get, src_zb, put):
        def merge(count, part):
            acc = None
            for j in range(count):
                v = part(j)
                v = pltpu.roll(v, (j - src_zb) % 128, 2) if j != src_zb else v
                acc = v if acc is None else jnp.where(lane_z == j, v, acc)
            return acc
        put(slice(0, XI), merge(ycut, lambda yi: get(slice(0, XI), yi)))
        if YI > ycut:
            put(slice(XI, XI + YI - ycut), merge(XI, lambda xi: get(xi, slice(ycut, YI))))

    def ghost_x(v, packed, j, low):
        dst = 0 if low else XB - 1
        moved = pltpu.roll(v, ZB if low else 128 - ZB, 2)
        move = (ZB * (dst - j)) % 128
        return jnp.where(lane_x == dst, pltpu.roll(packed, move, 2) if move else packed, moved)

    def ghost_z(v, packed, j, low):
        dst = 0 if low else ZB - 1
        moved = pltpu.roll(v, 1 if low else 127, 2)
        move = (dst - j) % 128
        return jnp.where(lane_z == dst, pltpu.roll(packed, move, 2) if move else packed, moved)

    def ghost_y(v, rows, low):
        dst = 0 if low else YB - 1
        moved = pltpu.roll(v, 1 if low else YB - 1, v.ndim - 2)
        return jnp.where(sub == dst, jnp.broadcast_to(rows, v.shape), moved)

    def pack_field(f, c, o):
        def put(ref, d):
            def put_(*v):
                ref[(d, c) + v[:-1]] = v[-1]
            return put_
        xa, za = slice(o, o + XI), slice(o, o + ZI)

        def line(i):
            return slice(i.start + o, i.stop + o) if isinstance(i, slice) else i + o
        pack_x(lambda yi: f[c, o, yi + o, za], 0, put(xs, 0))
        pack_x(lambda yi: f[c, XI - 1 + o, yi + o, za], ZB, put(xs, 1))
        pack_z(lambda xi, yi: f[c, line(xi), line(yi), o], 0, put(zs, 0))
        pack_z(lambda xi, yi: f[c, line(xi), line(yi), ZI - 1 + o], ZB - 1, put(zs, 1))
        ys[0, c] = f[c, xa, o, za, 0:1, :]
        ys[1, c] = f[c, xa, YI - 1 + o, za, YB - 1:YB, :]

    def ghost_field(f, c, w):
        for yi in range(YI):
            f[c, 0, yi + 1, zsl] = ghost_x(f[c, XI, yi + 1, zsl], xr[w, 0, c], yi, True)
            f[c, XI + 1, yi + 1, zsl] = ghost_x(f[c, 1, yi + 1, zsl], xr[w, 1, c], yi, False)
        for yi in range(ycut):
            f[c, xsl, yi + 1, 0] = ghost_z(f[c, xsl, yi + 1, ZI], zr[w, 0, c, :XI], yi, True)
            f[c, xsl, yi + 1, ZI + 1] = ghost_z(f[c, xsl, yi + 1, 1], zr[w, 1, c, :XI], yi, False)
        if YI > ycut:
            for xi in range(XI):
                f[c, xi + 1, ytail, 0] = ghost_z(f[c, xi + 1, ytail, ZI], zr[w, 0, c, XI:], xi, True)
                f[c, xi + 1, ytail, ZI + 1] = ghost_z(f[c, xi + 1, ytail, 1], zr[w, 1, c, XI:], xi, False)
        f[c, xsl, 0, zsl] = ghost_y(f[c, xsl, YI, zsl], yr[w, 0, c], True)
        f[c, xsl, YI + 1, zsl] = ghost_y(f[c, xsl, 1, zsl], yr[w, 1, c], False)

    lower = ((px > 0, (pz, py, px - 1)), (py > 0, (pz, py - 1, px)), (pz > 0, (pz - 1, py, px)))
    upper = ((px < nx_dev - 1, (pz, py, px + 1)), (py < ny_dev - 1, (pz, py + 1, px)), (pz < nz_dev - 1, (pz + 1, py, px)))

    def halo_copies(w):
        out = []
        for axis, (src, dst) in enumerate(((xs, xr), (ys, yr), (zs, zr))):
            for d in range(2):
                ok_send, dev = (lower, upper)[d][axis]
                ok_recv, _ = (upper, lower)[d][axis]
                cp = pltpu.make_async_remote_copy(
                    src_ref=src.at[d], dst_ref=dst.at[w, 1 - d], send_sem=halo_send.at[w, 2 * axis + d],
                    recv_sem=halo_recv.at[w, 2 * axis + d], device_id=dev, device_id_type=MESH)
                out.append((ok_send, ok_recv, cp))
        return out

    def k_copies():
        out = []
        for axis, (src, dst) in enumerate(((kxs, kxr), (kys, kyr), (kzs, kzr))):
            cp = pltpu.make_async_remote_copy(
                src_ref=src, dst_ref=dst, send_sem=k_send.at[axis], recv_sem=k_recv.at[axis],
                device_id=upper[axis][1], device_id_type=MESH)
            out.append((upper[axis][0], lower[axis][0], cp))
        return out

    def start_all(copies):
        for ok_send, _, cp in copies:
            pl.when(ok_send)(cp.start)

    def wait_all(copies):
        for ok_send, ok_recv, cp in copies:
            pl.when(ok_send)(cp.wait_send)
            pl.when(ok_recv)(cp.wait_recv)

    def send_dot(kind, c, acc):
        acc = jnp.sum(acc, axis=0)
        dots[kind, c, me] = jnp.sum(acc, axis=0, keepdims=True)
        each_other(lambda dev: pltpu.make_async_remote_copy(
            src_ref=dots.at[kind, c, me], dst_ref=dots.at[kind, c, me], send_sem=dot_send.at[kind, c],
            recv_sem=dot_recv.at[kind, c], device_id=dev, device_id_type=MESH).start())

    def wait_dot(kind, c):
        rows = dots.at[kind, c, pl.ds(0, n_dev - 1)]
        cp = pltpu.make_async_remote_copy(
            src_ref=rows, dst_ref=rows, send_sem=dot_send.at[kind, c], recv_sem=dot_recv.at[kind, c],
            device_id=(pz, py, px), device_id_type=MESH)
        cp.wait_recv()
        cp.wait_send()
        terms = [dots[kind, c, d] for d in range(n_dev)]
        while len(terms) > 1:
            terms = [terms[i] + terms[i + 1] for i in range(0, len(terms), 2)]
        total = jnp.sum(terms[0], axis=1, keepdims=True)
        return jnp.broadcast_to(total, (1, 128))

    def phase_a(c, beta):
        if beta is not None:
            beta = jnp.broadcast_to(beta, (8, 128))

        def new_p(*idx):
            if beta is not None:
                p[idx] = r[idx] + beta * p[idx]

        def head(yi):
            new_p(c, 0, yi + 1, zsl)
            new_p(c, 1, yi + 1, zsl)
        unrolled(YI, head)

        def plane(xi, acc):
            new_p(c, xi + 1, ysl, 0)
            new_p(c, xi + 1, ysl, ZI + 1)
            new_p(c, xi + 1, 0, zsl)
            new_p(c, xi + 1, YI + 1, zsl)

            def line(yi, carry):
                acc, py_lo, pc, ky_lo = carry
                new_p(c, xi + 2, yi + 1, zsl)
                py_hi = p[c, xi + 1, yi + 2, zsl]
                ky_hi = ky[c, xi, yi + 1]
                out = s[c, xi, yi] * pc - ky_lo * py_lo - ky_hi * py_hi
                out = out - kx[c, xi, yi] * p[c, xi, yi + 1, zsl]
                out = out - kz[c, xi, yi, :ZI] * p[c, xi + 1, yi + 1, :ZI]
                out = out - kz[c, xi, yi, 1:] * p[c, xi + 1, yi + 1, 2:]
                out = out - kx[c, xi + 1, yi] * p[c, xi + 2, yi + 1, zsl]
                q[c, xi, yi] = out
                return acc + pc * out, pc, py_hi, ky_hi
            carry = (acc, p[c, xi + 1, 0, zsl], p[c, xi + 1, 1, zsl], ky[c, xi, 0])
            return lax.fori_loop(0, YI, line, carry, unroll=True)[0]
        return lax.fori_loop(0, XI, plane, jnp.zeros((ZI, 8, 128), jnp.float32))

    def phase_b(c, alpha):
        if alpha is not None:
            alpha = jnp.broadcast_to(alpha, (8, 128))

        def plane(xi, acc):
            def line(yi, acc):
                step = q[c, xi, yi] if alpha is None else alpha * q[c, xi, yi]
                v = r[c, xi + 1, yi + 1, zsl] - step
                r[c, xi + 1, yi + 1, zsl] = v
                return acc + v * v
            return lax.fori_loop(0, YI, line, acc, unroll=True)
        return lax.fori_loop(0, XI, plane, jnp.zeros((ZI, 8, 128), jnp.float32))

    def phase_x(c, alpha):
        alpha = jnp.broadcast_to(alpha, (8, 128))

        def plane(xi, _):
            x[c, xi] = x[c, xi] + alpha * p[c, xi + 1, ysl, zsl]
            return 0
        lax.fori_loop(0, XI, plane, 0)

    def both(fn):
        def system(c, _):
            fn(c)
            return 0
        lax.fori_loop(0, 2, system, 0)

    def put_x(c, xi, yi, zi, v):
        p[c, xi + 1, yi + 1, zi + 1] = v
        x[c, xi, yi, zi] = v
    relayout(0, put_x)
    both(lambda c: pack_field(p, c, 1))

    def put_to(ref, ox, oy, oz):
        def put(c, xi, yi, zi, v):
            ref[c, xi + ox, yi + oy, zi + oz] = v
        return put

    def put_k(ref, c):
        def put_(*v):
            ref[(c,) + v[:-1]] = v[-1]
        return put_

    def edge(cond, v):
        return jnp.where(cond, 0.0, v)
    copies_x, copies_y, copies_z = k_copies()
    relayout(3, put_to(kz, 0, 0, 1))
    both(lambda c: pack_z(lambda xi, yi: kz[c, xi, yi, ZI], ZB - 1, put_k(kzs, c)))
    pl.semaphore_wait(barrier, n_dev - 1)
    start_all(halo_copies(1))
    start_all([copies_z])
    relayout(1, put_to(kx, 1, 0, 0))
    both(lambda c: pack_x(lambda yi: kx[c, XI, yi], ZB, put_k(kxs, c)))
    start_all([copies_x])
    relayout(2, put_to(ky, 0, 1, 0))
    for c in range(2):
        kys[c] = ky[c, :, YI, :, YB - 1:YB, :]
    start_all([copies_y])
    relayout(4, put_to(s, 0, 0, 0))
    relayout(5, put_to(r, 1, 1, 1))
    wait_all(halo_copies(1))
    both(lambda c: ghost_field(p, c, 1))
    wait_all([copies_z, copies_x, copies_y])

    def ghost_k(c):
        for yi in range(YI):
            v = kx[c, XI, yi]
            kx[c, 0, yi] = ghost_x(v, kxr[c], yi, True)
            kx[c, XI, yi] = edge(jnp.logical_and(lane_x == XB - 1, px == nx_dev - 1), v)
        for yi in range(ycut):
            kz[c, :, yi, 0] = ghost_z(kz[c, :, yi, ZI], kzr[c, :XI], yi, True)
        if YI > ycut:
            for xi in range(XI):
                kz[c, xi, ycut:, 0] = ghost_z(kz[c, xi, ycut:, ZI], kzr[c, XI:], xi, True)
        kz[c, :, :, ZI] = edge(jnp.logical_and(lane_z == ZB - 1, pz == nz_dev - 1), kz[c, :, :, ZI])
        v = ky[c, :, YI]
        ky[c, :, 0] = ghost_y(v, kyr[c], True)
        ky[c, :, YI] = edge(jnp.logical_and(sub == YB - 1, py == ny_dev - 1), v)

        def diagonal(xi, _):
            def line(yi):
                v = s[c, xi, yi] + (kx[c, xi, yi] + kx[c, xi + 1, yi]) + (ky[c, xi, yi] + ky[c, xi, yi + 1])
                s[c, xi, yi] = v + (kz[c, xi, yi, :ZI] + kz[c, xi, yi, 1:])
            unrolled(YI, line)
            return 0
        lax.fori_loop(0, XI, diagonal, 0)
    both(ghost_k)

    for c in range(2):
        phase_a(c, None)
        send_dot(1, c, phase_b(c, None))
    both(lambda c: pack_field(r, c, 1))
    start_all(halo_copies(0))
    rho[...] = jnp.ones(rho.shape, jnp.float32)
    hist[...] = jnp.zeros(hist.shape, jnp.float32)
    wait_all(halo_copies(0))
    both(lambda c: ghost_field(r, c, 0))

    def new_rho(c, k):
        total = wait_dot(1, c)
        ratio = total / rho[c]
        rho[c] = total
        hist[c] = jnp.where(row_lane == k, total, hist[c])
        return ratio

    def iteration(k, _):
        slot = 2 + lax.rem(k, 2)
        for c in range(2):
            beta = new_rho(c, k)
            beta = jnp.where(k == 0, 0.0, beta)
            send_dot(0, c, phase_a(c, beta))

        @pl.when(k < ITERS - 1)
        def _():
            both(lambda c: pack_field(q, c, 0))
            start_all(halo_copies(slot))
        alphas = []
        for c in range(2):
            alpha = rho[c] / wait_dot(0, c)
            alphas.append(alpha)
            send_dot(1, c, phase_b(c, alpha))
        for c in range(2):
            phase_x(c, alphas[c])

        @pl.when(k < ITERS - 1)
        def _():
            wait_all(halo_copies(slot))
            for ref in (xr, yr, zr):
                for d in range(2):
                    for c in range(2):
                        ref[0, d, c] = ref[0, d, c] - alphas[c] * ref[slot, d, c]
            both(lambda c: ghost_field(r, c, 0))
        return 0
    lax.fori_loop(0, ITERS, iteration, 0)

    for c in range(2):
        pltpu.make_async_copy(x.at[c], xo_hbm.at[c], out_sem.at[c]).start()
    for c in range(2):
        new_rho(c, ITERS)
        hist_ref[c:c + 1, :] = jnp.sqrt(hist[c] / cells)[:, :ITERS + 1]
    for c in range(2):
        pltpu.make_async_copy(x.at[c], xo_hbm.at[c], out_sem.at[c]).wait()


def cell_order(dims, x_hbm, hist_in, o_hbm, hist_out, x, stage, tmp, hist, in_sem, out_sem, hist_sem):
    XI, YI, ZI = dims

    def in_copy(c, xi):
        return pltpu.make_async_copy(x_hbm.at[c, xi], x.at[c, xi], in_sem.at[c, xi])

    def out_copy(c, xi):
        return pltpu.make_async_copy(stage.at[c, :, xi], o_hbm.at[c, :, xi], out_sem.at[c, xi])
    hist_copies = pltpu.make_async_copy(hist_in, hist, hist_sem.at[0]), pltpu.make_async_copy(hist, hist_out, hist_sem.at[1])

    for c in range(2):
        for xi in range(XI):
            in_copy(c, xi).start()
    hist_copies[0].start()
    for c in range(2):
        for xi in range(XI):
            in_copy(c, xi).wait()

        def plane(xi, _):
            def gather(zi, _):
                for yi in range(YI):
                    tmp[xi * ZI + zi, pl.ds(yi, YB, stride=YI), :] = x[c, xi, yi, zi]
                return 0
            lax.fori_loop(0, ZI, gather, 0, unroll=True)

            def put(zi, _):
                stage[c, :, xi, pl.ds(zi, ZB, stride=ZI), :] = tmp[xi * ZI + zi].T.reshape(XB, ZB, tmp.shape[1])
                return 0
            lax.fori_loop(0, ZI, put, 0, unroll=True)
            out_copy(c, xi).start()
            return 0
        lax.fori_loop(0, XI, plane, 0, unroll=True)
        if c == 0:
            hist_copies[0].wait()
            hist_copies[1].start()
    for c in range(2):
        for xi in range(XI):
            out_copy(c, xi).wait()
    hist_copies[1].wait()


def solution(mesh):
    sizes = tuple(mesh.shape[a] for a in AXES)
    n_dev = sizes[0] * sizes[1] * sizes[2]
    field_spec = P(None, 'px', 'py', 'pz')

    def local_solve(*args):
        _, nx, ny, nz = args[0].shape
        XI, YI, ZI = nx // XB, ny // YB, nz // ZB
        cells = float(nx * ny * nz * n_dev)
        f32 = jnp.float32
        rows = (XI, ZI, 1, 128)
        mz = XI + max(0, YI - ZB)

        def vregs(*lead):
            return pltpu.VMEM(lead + (8, 128), f32)
        hbm = pl.BlockSpec(memory_space=pl.ANY)
        args = [jnp.swapaxes(a, 2, 3).reshape(2, XB, XI, nz, ny) for a in args]
        x_out, hist = pl.pallas_call(
            functools.partial(kernel, sizes, (XI, YI, ZI, cells)),
            out_shape=(jax.ShapeDtypeStruct((2, XI, YI, ZI, 8, 128), f32), jax.ShapeDtypeStruct((2, ITERS + 1), f32)),
            in_specs=[hbm] * 6,
            out_specs=(hbm, pl.BlockSpec(memory_space=pltpu.VMEM)),
            scratch_shapes=[
                pltpu.VMEM((6, 2, XB, XI, nz, ny), f32),
                vregs(2, XI + 2, YI + 2, ZI + 2), vregs(2, XI + 2, YI + 2, ZI + 2),
                vregs(2, XI, YI, ZI), vregs(2, XI, YI, ZI), vregs(2, XI, YI, ZI),
                vregs(2, XI + 1, YI, ZI), vregs(2, XI, YI + 1, ZI), vregs(2, XI, YI, ZI + 1),
                pltpu.VMEM((XI * ZI // 2, ny, 128), f32),
                vregs(2, 2, ZI), vregs(4, 2, 2, ZI), pltpu.VMEM((2, 2) + rows, f32), pltpu.VMEM((4, 2, 2) + rows, f32),
                vregs(2, 2, mz), vregs(4, 2, 2, mz),
                vregs(2, ZI), vregs(2, ZI), pltpu.VMEM((2,) + rows, f32), pltpu.VMEM((2,) + rows, f32),
                vregs(2, mz), vregs(2, mz),
                pltpu.VMEM((2, 2, n_dev, 1, 128), f32), pltpu.VMEM((2, 1, 128), f32), pltpu.VMEM((2, 1, 128), f32),
                pltpu.SemaphoreType.DMA((6, 2)), pltpu.SemaphoreType.DMA((2,)),
                pltpu.SemaphoreType.DMA((2, 2)), pltpu.SemaphoreType.DMA((2, 2)),
                pltpu.SemaphoreType.DMA((4, 6)), pltpu.SemaphoreType.DMA((4, 6)),
                pltpu.SemaphoreType.DMA((3,)), pltpu.SemaphoreType.DMA((3,)),
            ],
            compiler_params=pltpu.CompilerParams(collective_id=0, has_side_effects=True, vmem_limit_bytes=67043328),
            name='cg',
        )(*args)
        x_out, hist = pl.pallas_call(
            functools.partial(cell_order, (XI, YI, ZI)),
            out_shape=(jax.ShapeDtypeStruct((2, XB, XI, nz, ny), f32), jax.ShapeDtypeStruct(hist.shape, f32)),
            in_specs=[hbm, hbm], out_specs=(hbm, hbm),
            scratch_shapes=[
                vregs(2, XI, YI, ZI), pltpu.VMEM((2, XB, XI, nz, ny), f32), pltpu.VMEM((XI * ZI, ny, 128), f32),
                pltpu.VMEM(hist.shape, f32),
                pltpu.SemaphoreType.DMA((2, XI)), pltpu.SemaphoreType.DMA((2, XI)), pltpu.SemaphoreType.DMA((2,)),
            ],
            compiler_params=pltpu.CompilerParams(vmem_limit_bytes=67043328),
            name='cell_order',
        )(x_out, hist)
        return jnp.swapaxes(x_out.reshape(2, nx, nz, ny), 2, 3), hist

    return jax.shard_map(local_solve, mesh=mesh, in_specs=(field_spec,) * 6, out_specs=(field_spec, P(None, None)), check_vma=False)
```

```python
import functools

import jax
import jax.numpy as jnp
from jax import lax
from jax.experimental import pallas as pl
from jax.experimental.pallas import tpu as pltpu
from jax.sharding import PartitionSpec as P

ITERS = 20
AXES = ('pz', 'py', 'px')
MESH = pl.DeviceIdType.MESH
XB, YB, ZB = 16, 8, 8


def kernel(sizes, dims, s_hbm, b_hbm, x_hbm, kx_hbm, ky_hbm, kz_hbm, xo_hbm, hist_ref,
           stage, r, p, q, x, s, kx, ky, kz, tmp,
           xs, xr, ys, yr, zs, zr, kxs, kxr, kys, kyr, kzs, kzr,
           dots, rho, hist,
           in_sem, out_sem, dot_send, dot_recv, halo_send, halo_recv, k_send, k_recv):
    nz_dev, ny_dev, nx_dev = sizes
    n_dev = nz_dev * ny_dev * nx_dev
    XI, YI, ZI, cells = dims
    pz, py, px = (lax.axis_index(a) for a in AXES)
    me = (pz * ny_dev + py) * nx_dev + px
    lane = lax.broadcasted_iota(jnp.int32, (8, 128), 1)
    sub = lax.broadcasted_iota(jnp.int32, (8, 128), 0)
    lane_z = lax.rem(lane, ZB)
    lane_x = lax.div(lane, ZB)
    row_lane = lax.broadcasted_iota(jnp.int32, (1, 128), 1)

    arrays = (x_hbm, kx_hbm, ky_hbm, kz_hbm, s_hbm, b_hbm)

    def in_copy(a, c):
        return pltpu.make_async_copy(arrays[a].at[c], stage.at[a, c], in_sem.at[a, c])

    for a in (0, 3, 1, 2, 4, 5):
        for c in range(2):
            in_copy(a, c).start()

    for ref in (xr, yr, zr, kxr, kyr, kzr):
        ref[...] = jnp.zeros(ref.shape, ref.dtype)

    def far_first(pos, size, n):
        high = lax.div(2 * pos, size)
        return high * n + (1 - high) * (size - 1 - n)

    others = []
    for n in range(n_dev):
        dev = (far_first(pz, nz_dev, n // (ny_dev * nx_dev)), far_first(py, ny_dev, n // nx_dev % ny_dev),
               far_first(lax.div(px, 2), nx_dev // 2, n % nx_dev // 2) * 2 + n % 2)
        others.append((dev, (dev[0] * ny_dev + dev[1]) * nx_dev + dev[2] != me))

    def each_other(fn):
        for dev, is_other in others:
            pl.when(is_other)(functools.partial(fn, dev))

    barrier = pltpu.get_barrier_semaphore()
    each_other(lambda dev: pl.semaphore_signal(barrier, inc=1, device_id=dev, device_id_type=MESH))

    def unrolled(n, fn):
        def step(i, _):
            fn(i)
            return 0
        lax.fori_loop(0, n, step, 0, unroll=True)

    ysl, zsl = slice(1, YI + 1), slice(1, ZI + 1)
    xsl = slice(1, XI + 1)
    ytail = slice(min(YI, ZB) + 1, YI + 1)

    def block(half, i):
        n = half * (XI * ZI // 2) + i
        return lax.div(n, ZI), lax.rem(n, ZI)

    def relayout(a, stores):
        def system(c, _):
            in_copy(a, c).wait()

            def chunk(half, _):
                def load(i):
                    xi, zi = block(half, i)
                    rows = stage[a, c, :, xi, pl.ds(zi, ZB, stride=ZI), :]
                    tmp[i] = rows.reshape(128, rows.shape[-1]).T

                def store(i):
                    xi, zi = block(half, i)
                    unrolled(YI, lambda yi: stores(c, xi, yi, zi, tmp[i, pl.ds(yi, YB, stride=YI), :]))
                unrolled(XI * ZI // 2, load)
                unrolled(XI * ZI // 2, store)
                return 0
            return lax.fori_loop(0, 2, chunk, 0)
        lax.fori_loop(0, 2, system, 0)

    def pack_x(get, shift, put):
        acc = pltpu.roll(get(0), shift, 2) if shift else get(0)
        for j in range(1, YI):
            acc = jnp.where(lane_x == j, pltpu.roll(get(j), (shift + ZB * j) % 128, 2), acc)
        put(acc)

    ycut = min(YI, ZB)

    def pack_z(get, src_zb, put):
        def merge(count, part):
            acc = None
            for j in range(count):
                v = part(j)
                v = pltpu.roll(v, (j - src_zb) % 128, 2) if j != src_zb else v
                acc = v if acc is None else jnp.where(lane_z == j, v, acc)
            return acc
        put(slice(0, XI), merge(ycut, lambda yi: get(slice(0, XI), yi)))
        if YI > ycut:
            put(slice(XI, XI + YI - ycut), merge(XI, lambda xi: get(xi, slice(ycut, YI))))

    def ghost_x(v, packed, j, low):
        dst = 0 if low else XB - 1
        moved = pltpu.roll(v, ZB if low else 128 - ZB, 2)
        move = (ZB * (dst - j)) % 128
        return jnp.where(lane_x == dst, pltpu.roll(packed, move, 2) if move else packed, moved)

    def ghost_z(v, packed, j, low):
        dst = 0 if low else ZB - 1
        moved = pltpu.roll(v, 1 if low else 127, 2)
        move = (dst - j) % 128
        return jnp.where(lane_z == dst, pltpu.roll(packed, move, 2) if move else packed, moved)

    def ghost_y(v, rows, low):
        dst = 0 if low else YB - 1
        moved = pltpu.roll(v, 1 if low else YB - 1, v.ndim - 2)
        return jnp.where(sub == dst, jnp.broadcast_to(rows, v.shape), moved)

    def pack_field(f, c, o):
        def put(ref, d):
            def put_(*v):
                ref[(d, c) + v[:-1]] = v[-1]
            return put_
        xa, za = slice(o, o + XI), slice(o, o + ZI)

        def line(i):
            return slice(i.start + o, i.stop + o) if isinstance(i, slice) else i + o
        pack_x(lambda yi: f[c, o, yi + o, za], 0, put(xs, 0))
        pack_x(lambda yi: f[c, XI - 1 + o, yi + o, za], ZB, put(xs, 1))
        pack_z(lambda xi, yi: f[c, line(xi), line(yi), o], 0, put(zs, 0))
        pack_z(lambda xi, yi: f[c, line(xi), line(yi), ZI - 1 + o], ZB - 1, put(zs, 1))
        ys[0, c] = f[c, xa, o, za, 0:1, :]
        ys[1, c] = f[c, xa, YI - 1 + o, za, YB - 1:YB, :]

    def ghost_field(f, c, w):
        for yi in range(YI):
            f[c, 0, yi + 1, zsl] = ghost_x(f[c, XI, yi + 1, zsl], xr[w, 0, c], yi, True)
            f[c, XI + 1, yi + 1, zsl] = ghost_x(f[c, 1, yi + 1, zsl], xr[w, 1, c], yi, False)
        for yi in range(ycut):
            f[c, xsl, yi + 1, 0] = ghost_z(f[c, xsl, yi + 1, ZI], zr[w, 0, c, :XI], yi, True)
            f[c, xsl, yi + 1, ZI + 1] = ghost_z(f[c, xsl, yi + 1, 1], zr[w, 1, c, :XI], yi, False)
        if YI > ycut:
            for xi in range(XI):
                f[c, xi + 1, ytail, 0] = ghost_z(f[c, xi + 1, ytail, ZI], zr[w, 0, c, XI:], xi, True)
                f[c, xi + 1, ytail, ZI + 1] = ghost_z(f[c, xi + 1, ytail, 1], zr[w, 1, c, XI:], xi, False)
        f[c, xsl, 0, zsl] = ghost_y(f[c, xsl, YI, zsl], yr[w, 0, c], True)
        f[c, xsl, YI + 1, zsl] = ghost_y(f[c, xsl, 1, zsl], yr[w, 1, c], False)

    lower = ((px > 0, (pz, py, px - 1)), (py > 0, (pz, py - 1, px)), (pz > 0, (pz - 1, py, px)))
    upper = ((px < nx_dev - 1, (pz, py, px + 1)), (py < ny_dev - 1, (pz, py + 1, px)), (pz < nz_dev - 1, (pz + 1, py, px)))

    def halo_copies(w):
        out = []
        for axis, (src, dst) in enumerate(((xs, xr), (ys, yr), (zs, zr))):
            for d in range(2):
                ok_send, dev = (lower, upper)[d][axis]
                ok_recv, _ = (upper, lower)[d][axis]
                cp = pltpu.make_async_remote_copy(
                    src_ref=src.at[d], dst_ref=dst.at[w, 1 - d], send_sem=halo_send.at[w, 2 * axis + d],
                    recv_sem=halo_recv.at[w, 2 * axis + d], device_id=dev, device_id_type=MESH)
                out.append((ok_send, ok_recv, cp))
        return out

    def k_copies():
        out = []
        for axis, (src, dst) in enumerate(((kxs, kxr), (kys, kyr), (kzs, kzr))):
            cp = pltpu.make_async_remote_copy(
                src_ref=src, dst_ref=dst, send_sem=k_send.at[axis], recv_sem=k_recv.at[axis],
                device_id=upper[axis][1], device_id_type=MESH)
            out.append((upper[axis][0], lower[axis][0], cp))
        return out

    def start_all(copies):
        for ok_send, _, cp in copies:
            pl.when(ok_send)(cp.start)

    def wait_all(copies):
        for ok_send, ok_recv, cp in copies:
            pl.when(ok_send)(cp.wait_send)
            pl.when(ok_recv)(cp.wait_recv)

    def send_dot(kind, c, acc):
        acc = jnp.sum(acc, axis=0)
        dots[kind, c, me] = jnp.sum(acc, axis=0, keepdims=True)
        each_other(lambda dev: pltpu.make_async_remote_copy(
            src_ref=dots.at[kind, c, me], dst_ref=dots.at[kind, c, me], send_sem=dot_send.at[kind, c],
            recv_sem=dot_recv.at[kind, c], device_id=dev, device_id_type=MESH).start())

    def wait_dot(kind, c):
        rows = dots.at[kind, c, pl.ds(0, n_dev - 1)]
        cp = pltpu.make_async_remote_copy(
            src_ref=rows, dst_ref=rows, send_sem=dot_send.at[kind, c], recv_sem=dot_recv.at[kind, c],
            device_id=(pz, py, px), device_id_type=MESH)
        cp.wait_recv()
        cp.wait_send()
        terms = [dots[kind, c, d] for d in range(n_dev)]
        while len(terms) > 1:
            terms = [terms[i] + terms[i + 1] for i in range(0, len(terms), 2)]
        total = jnp.sum(terms[0], axis=1, keepdims=True)
        return jnp.broadcast_to(total, (1, 128))

    def phase_a(c, beta):
        if beta is not None:
            beta = jnp.broadcast_to(beta, (8, 128))

        def new_p(*idx):
            if beta is not None:
                p[idx] = r[idx] + beta * p[idx]

        def head(yi):
            new_p(c, 0, yi + 1, zsl)
            new_p(c, 1, yi + 1, zsl)
        unrolled(YI, head)

        def plane(xi, acc):
            new_p(c, xi + 1, ysl, 0)
            new_p(c, xi + 1, ysl, ZI + 1)
            new_p(c, xi + 1, 0, zsl)
            new_p(c, xi + 1, YI + 1, zsl)

            def line(yi, carry):
                acc, py_lo, pc, ky_lo = carry
                new_p(c, xi + 2, yi + 1, zsl)
                py_hi = p[c, xi + 1, yi + 2, zsl]
                ky_hi = ky[c, xi, yi + 1]
                out = s[c, xi, yi] * pc - ky_lo * py_lo - ky_hi * py_hi
                out = out - kx[c, xi, yi] * p[c, xi, yi + 1, zsl]
                out = out - kz[c, xi, yi, :ZI] * p[c, xi + 1, yi + 1, :ZI]
                out = out - kz[c, xi, yi, 1:] * p[c, xi + 1, yi + 1, 2:]
                out = out - kx[c, xi + 1, yi] * p[c, xi + 2, yi + 1, zsl]
                q[c, xi, yi] = out
                return acc + pc * out, pc, py_hi, ky_hi
            carry = (acc, p[c, xi + 1, 0, zsl], p[c, xi + 1, 1, zsl], ky[c, xi, 0])
            return lax.fori_loop(0, YI, line, carry, unroll=True)[0]
        return lax.fori_loop(0, XI, plane, jnp.zeros((ZI, 8, 128), jnp.float32))

    def phase_b(c, alpha):
        if alpha is not None:
            alpha = jnp.broadcast_to(alpha, (8, 128))

        def plane(xi, acc):
            def line(yi, acc):
                step = q[c, xi, yi] if alpha is None else alpha * q[c, xi, yi]
                v = r[c, xi + 1, yi + 1, zsl] - step
                r[c, xi + 1, yi + 1, zsl] = v
                return acc + v * v
            return lax.fori_loop(0, YI, line, acc, unroll=True)
        return lax.fori_loop(0, XI, plane, jnp.zeros((ZI, 8, 128), jnp.float32))

    def phase_x(c, alpha):
        alpha = jnp.broadcast_to(alpha, (8, 128))

        def plane(xi, _):
            x[c, xi] = x[c, xi] + alpha * p[c, xi + 1, ysl, zsl]
            return 0
        lax.fori_loop(0, XI, plane, 0)

    def both(fn):
        def system(c, _):
            fn(c)
            return 0
        lax.fori_loop(0, 2, system, 0)

    def put_x(c, xi, yi, zi, v):
        p[c, xi + 1, yi + 1, zi + 1] = v
        x[c, xi, yi, zi] = v
    relayout(0, put_x)
    both(lambda c: pack_field(p, c, 1))

    def put_to(ref, ox, oy, oz):
        def put(c, xi, yi, zi, v):
            ref[c, xi + ox, yi + oy, zi + oz] = v
        return put

    def put_k(ref, c):
        def put_(*v):
            ref[(c,) + v[:-1]] = v[-1]
        return put_

    def edge(cond, v):
        return jnp.where(cond, 0.0, v)
    copies_x, copies_y, copies_z = k_copies()
    relayout(3, put_to(kz, 0, 0, 1))
    both(lambda c: pack_z(lambda xi, yi: kz[c, xi, yi, ZI], ZB - 1, put_k(kzs, c)))
    pl.semaphore_wait(barrier, n_dev - 1)
    start_all(halo_copies(1))
    start_all([copies_z])
    relayout(1, put_to(kx, 1, 0, 0))
    both(lambda c: pack_x(lambda yi: kx[c, XI, yi], ZB, put_k(kxs, c)))
    start_all([copies_x])
    relayout(2, put_to(ky, 0, 1, 0))
    for c in range(2):
        kys[c] = ky[c, :, YI, :, YB - 1:YB, :]
    start_all([copies_y])
    relayout(4, put_to(s, 0, 0, 0))
    relayout(5, put_to(r, 1, 1, 1))
    wait_all(halo_copies(1))
    both(lambda c: ghost_field(p, c, 1))
    wait_all([copies_z, copies_x, copies_y])

    def ghost_k(c):
        for yi in range(YI):
            v = kx[c, XI, yi]
            kx[c, 0, yi] = ghost_x(v, kxr[c], yi, True)
            kx[c, XI, yi] = edge(jnp.logical_and(lane_x == XB - 1, px == nx_dev - 1), v)
        for yi in range(ycut):
            kz[c, :, yi, 0] = ghost_z(kz[c, :, yi, ZI], kzr[c, :XI], yi, True)
        if YI > ycut:
            for xi in range(XI):
                kz[c, xi, ycut:, 0] = ghost_z(kz[c, xi, ycut:, ZI], kzr[c, XI:], xi, True)
        kz[c, :, :, ZI] = edge(jnp.logical_and(lane_z == ZB - 1, pz == nz_dev - 1), kz[c, :, :, ZI])
        v = ky[c, :, YI]
        ky[c, :, 0] = ghost_y(v, kyr[c], True)
        ky[c, :, YI] = edge(jnp.logical_and(sub == YB - 1, py == ny_dev - 1), v)

        def diagonal(xi, _):
            def line(yi):
                v = s[c, xi, yi] + (kx[c, xi, yi] + kx[c, xi + 1, yi]) + (ky[c, xi, yi] + ky[c, xi, yi + 1])
                s[c, xi, yi] = v + (kz[c, xi, yi, :ZI] + kz[c, xi, yi, 1:])
            unrolled(YI, line)
            return 0
        lax.fori_loop(0, XI, diagonal, 0)
    both(ghost_k)

    for c in range(2):
        phase_a(c, None)
        send_dot(1, c, phase_b(c, None))
    both(lambda c: pack_field(r, c, 1))
    start_all(halo_copies(0))
    rho[...] = jnp.ones(rho.shape, jnp.float32)
    hist[...] = jnp.zeros(hist.shape, jnp.float32)
    wait_all(halo_copies(0))
    both(lambda c: ghost_field(r, c, 0))

    def new_rho(c, k):
        total = wait_dot(1, c)
        ratio = total / rho[c]
        rho[c] = total
        hist[c] = jnp.where(row_lane == k, total, hist[c])
        return ratio

    def iteration(k, _):
        slot = 2 + lax.rem(k, 2)
        for c in range(2):
            beta = new_rho(c, k)
            beta = jnp.where(k == 0, 0.0, beta)
            send_dot(0, c, phase_a(c, beta))

        @pl.when(k < ITERS - 1)
        def _():
            both(lambda c: pack_field(q, c, 0))
            start_all(halo_copies(slot))
        alphas = []
        for c in range(2):
            alpha = rho[c] / wait_dot(0, c)
            alphas.append(alpha)
            send_dot(1, c, phase_b(c, alpha))
        for c in range(2):
            phase_x(c, alphas[c])

        @pl.when(k < ITERS - 1)
        def _():
            wait_all(halo_copies(slot))
            for ref in (xr, yr, zr):
                for d in range(2):
                    for c in range(2):
                        ref[0, d, c] = ref[0, d, c] - alphas[c] * ref[slot, d, c]
            both(lambda c: ghost_field(r, c, 0))
        return 0
    lax.fori_loop(0, ITERS, iteration, 0)

    for c in range(2):
        pltpu.make_async_copy(x.at[c], xo_hbm.at[c], out_sem.at[c]).start()
    for c in range(2):
        new_rho(c, ITERS)
        hist_ref[c:c + 1, :] = jnp.sqrt(hist[c] / cells)[:, :ITERS + 1]
    for c in range(2):
        pltpu.make_async_copy(x.at[c], xo_hbm.at[c], out_sem.at[c]).wait()


def cell_order(dims, x_hbm, hist_in, o_hbm, hist_out, x, stage, tmp, hist, in_sem, out_sem, hist_sem):
    XI, YI, ZI = dims

    def in_copy(c, xi):
        return pltpu.make_async_copy(x_hbm.at[c, xi], x.at[c, xi], in_sem.at[c, xi])

    def out_copy(c, xi):
        return pltpu.make_async_copy(stage.at[c, :, xi], o_hbm.at[c, :, xi], out_sem.at[c, xi])
    hist_copies = pltpu.make_async_copy(hist_in, hist, hist_sem.at[0]), pltpu.make_async_copy(hist, hist_out, hist_sem.at[1])

    for c in range(2):
        for xi in range(XI):
            in_copy(c, xi).start()
    hist_copies[0].start()
    for c in range(2):
        for xi in range(XI):
            in_copy(c, xi).wait()

        def plane(xi, _):
            def gather(zi, _):
                for yi in range(YI):
                    tmp[xi * ZI + zi, pl.ds(yi, YB, stride=YI), :] = x[c, xi, yi, zi]
                return 0
            lax.fori_loop(0, ZI, gather, 0, unroll=True)

            def put(zi, _):
                stage[c, :, xi, pl.ds(zi, ZB, stride=ZI), :] = tmp[xi * ZI + zi].T.reshape(XB, ZB, tmp.shape[1])
                return 0
            lax.fori_loop(0, ZI, put, 0, unroll=True)
            out_copy(c, xi).start()
            return 0
        lax.fori_loop(0, XI, plane, 0, unroll=True)
        if c == 0:
            hist_copies[0].wait()
            hist_copies[1].start()
    for c in range(2):
        for xi in range(XI):
            out_copy(c, xi).wait()
    hist_copies[1].wait()


def solution(mesh):
    sizes = tuple(mesh.shape[a] for a in AXES)
    n_dev = sizes[0] * sizes[1] * sizes[2]
    field_spec = P(None, 'px', 'py', 'pz')

    def local_solve(*args):
        _, nx, ny, nz = args[0].shape
        XI, YI, ZI = nx // XB, ny // YB, nz // ZB
        cells = float(nx * ny * nz * n_dev)
        f32 = jnp.float32
        rows = (XI, ZI, 1, 128)
        mz = XI + max(0, YI - ZB)

        def vregs(*lead):
            return pltpu.VMEM(lead + (8, 128), f32)
        hbm = pl.BlockSpec(memory_space=pl.ANY)
        args = [jnp.swapaxes(a, 2, 3).reshape(2, XB, XI, nz, ny) for a in args]
        x_out, hist = pl.pallas_call(
            functools.partial(kernel, sizes, (XI, YI, ZI, cells)),
            out_shape=(jax.ShapeDtypeStruct((2, XI, YI, ZI, 8, 128), f32), jax.ShapeDtypeStruct((2, ITERS + 1), f32)),
            in_specs=[hbm] * 6,
            out_specs=(hbm, pl.BlockSpec(memory_space=pltpu.VMEM)),
            scratch_shapes=[
                pltpu.VMEM((6, 2, XB, XI, nz, ny), f32),
                vregs(2, XI + 2, YI + 2, ZI + 2), vregs(2, XI + 2, YI + 2, ZI + 2),
                vregs(2, XI, YI, ZI), vregs(2, XI, YI, ZI), vregs(2, XI, YI, ZI),
                vregs(2, XI + 1, YI, ZI), vregs(2, XI, YI + 1, ZI), vregs(2, XI, YI, ZI + 1),
                pltpu.VMEM((XI * ZI // 2, ny, 128), f32),
                vregs(2, 2, ZI), vregs(4, 2, 2, ZI), pltpu.VMEM((2, 2) + rows, f32), pltpu.VMEM((4, 2, 2) + rows, f32),
                vregs(2, 2, mz), vregs(4, 2, 2, mz),
                vregs(2, ZI), vregs(2, ZI), pltpu.VMEM((2,) + rows, f32), pltpu.VMEM((2,) + rows, f32),
                vregs(2, mz), vregs(2, mz),
                pltpu.VMEM((2, 2, n_dev, 1, 128), f32), pltpu.VMEM((2, 1, 128), f32), pltpu.VMEM((2, 1, 128), f32),
                pltpu.SemaphoreType.DMA((6, 2)), pltpu.SemaphoreType.DMA((2,)),
                pltpu.SemaphoreType.DMA((2, 2)), pltpu.SemaphoreType.DMA((2, 2)),
                pltpu.SemaphoreType.DMA((4, 6)), pltpu.SemaphoreType.DMA((4, 6)),
                pltpu.SemaphoreType.DMA((3,)), pltpu.SemaphoreType.DMA((3,)),
            ],
            compiler_params=pltpu.CompilerParams(collective_id=0, has_side_effects=True, vmem_limit_bytes=67043328),
            name='cg',
        )(*args)
        x_out, hist = pl.pallas_call(
            functools.partial(cell_order, (XI, YI, ZI)),
            out_shape=(jax.ShapeDtypeStruct((2, XB, XI, nz, ny), f32), jax.ShapeDtypeStruct(hist.shape, f32)),
            in_specs=[hbm, hbm], out_specs=(hbm, hbm),
            scratch_shapes=[
                vregs(2, XI, YI, ZI), pltpu.VMEM((2, XB, XI, nz, ny), f32), pltpu.VMEM((XI * ZI, ny, 128), f32),
                pltpu.VMEM(hist.shape, f32),
                pltpu.SemaphoreType.DMA((2, XI)), pltpu.SemaphoreType.DMA((2, XI)), pltpu.SemaphoreType.DMA((2,)),
            ],
            compiler_params=pltpu.CompilerParams(vmem_limit_bytes=67043328),
            name='cell_order',
        )(x_out, hist)
        return jnp.swapaxes(x_out.reshape(2, nx, nz, ny), 2, 3), hist

    return jax.shard_map(local_solve, mesh=mesh, in_specs=(field_spec,) * 6, out_specs=(field_spec, P(None, None)), check_vma=False)
```
